128 devices in a mesh: gx: 4 (over y), gz: 32 (over x, z, core).
Axes of the slice: x: 4, y: 4, z: 4, core: 2. Of those that a mesh axis runs over, the one named last changes fastest.
Arguments:
- divergence: float32 [256, 512, 512], P('gx', 'gz'), may hold values from -18 to 18
- level_set: float32 [256, 512, 512], P('gx', 'gz'), may hold values from -2 to 2, as said below
- tile_ids: int32 [4, 32768], P('gx', 'gz'), may hold values from -1 to 1023, as said below
Outputs:
- pressure: float32 [256, 512, 512], P('gx', 'gz')
- residual: float32 [256, 512, 512], P('gx', 'gz')
The draws below stay inside these ranges and needn't reach their ends.
Inputs may be any that keep to these rules, and one draw needn't show every extreme that they name: `level_set`: every entry lies at least 0.05 away from zero. `tile_ids`: each device's part lists distinct tile numbers of its own block, below 1024, in increasing order, followed by -1 entries; some device lists all 1024 and some device lists none.
All inputs are finite; a program needn't handle non-finite values.
Results may differ from the reference program's by a relative error of at most 0.0003.
Values sent between devices are 32-bit elements; how exact they have to be, the bound alone decides.
A program may use at most 128 MiB of HBM per device.

```python
import math
import jax
import jax.numpy as jnp
from jax import lax

CX = 64
CZ = 16
NY = 512
ITERS = 2
TILE = 8
NX = 256
NZ = 512
TILES_DEV = 1024
SLOTS = 1024
N_GX = 4
N_GZ = 32


def surface_height(key):
    lowest = 35 * NZ // 100
    highest = 75 * NZ // 100
    return jax.random.randint(jax.random.fold_in(key, 12), (NX, NY), lowest, highest).astype(jnp.int32)


def draw_level_set(key, part):
    shape = (NX, NZ, NY)
    mag_key = jax.random.fold_in(key, 11)
    flip_key = jax.random.fold_in(key, 13)
    magnitude = jnp.exp(jax.random.uniform(mag_key, shape, jnp.float32, math.log(0.05), math.log(2.0)))
    magnitude = jnp.clip(magnitude, 0.05, 2.0)
    height = surface_height(key)[:, None, :]
    levels = lax.broadcasted_iota(jnp.int32, (1, NZ, 1), 1)
    bulk = levels < height
    nearby = jnp.abs(levels - height) <= 3
    flipped = jnp.logical_and(nearby, jax.random.randint(flip_key, shape, 0, 10) == 0)
    inside = jnp.logical_xor(bulk, flipped)
    return jnp.where(inside, -magnitude, magnitude)


def draw_tile_ids(key, part):
    devices = N_GX * N_GZ
    counts = jax.random.randint(jax.random.fold_in(key, 21), (devices,), 0, TILES_DEV + 1).astype(jnp.int32)
    device_order = jax.random.permutation(jax.random.fold_in(key, 22), devices).astype(jnp.int32)
    counts = jnp.where(device_order == 0, TILES_DEV, jnp.where(device_order == 1, 0, counts)).astype(jnp.int32)
    device_keys = jax.random.split(jax.random.fold_in(key, 23), devices)
    ranking = jax.vmap(lambda single: jax.random.permutation(single, TILES_DEV))(device_keys).astype(jnp.int32)
    chosen = ranking < counts[:, None]
    numbers = lax.broadcasted_iota(jnp.int32, (devices, TILES_DEV), 1)
    scores = jnp.where(chosen, numbers, numbers + TILES_DEV).astype(jnp.int32)
    ordered = jnp.sort(scores, axis=1)
    listed = jnp.where(ordered < TILES_DEV, ordered, -1).astype(jnp.int32)
    return listed.reshape(N_GX, N_GZ * SLOTS).astype(jnp.int32)


def block_scale(stream_key, shape, cuts, least, top_value):
    level, own = 1.0, jax.random.fold_in(stream_key, 6)
    for position, parts in cuts:
        draws = jnp.exp(jax.random.uniform(jax.random.fold_in(own, position), (parts,), jnp.float32, least / len(cuts), top_value / len(cuts)))
        level = level * jnp.repeat(draws, shape[position] // parts).reshape([-1 if axis == position else 1 for axis in range(len(shape))])
    return level


def centred(rng, extent, deviation, most, cuts=(), held_as=jnp.bfloat16):
    drawn = jax.random.normal(rng, extent, jnp.float32) * deviation
    if len(cuts) > 0:
        drawn = block_scale(rng, extent, cuts, -0.22, 0.18) * drawn
    return jnp.clip(drawn, min=-most, max=most).astype(held_as)


def setup_inputs(seed: int = 0) -> dict:
    key_of = jax.random.split(jax.random.key(seed), 4)
    divergence = centred(key_of[0], (NX, NZ, NY), 3.0, 18.0, ((0, 4), (1, 32)), jnp.float32)
    level_set = draw_level_set(jax.random.fold_in(key_of[3], 71), 0)
    tile_ids = draw_tile_ids(jax.random.fold_in(key_of[3], 71), 0)
    return dict(divergence=divergence, level_set=level_set, tile_ids=tile_ids)


damping = 2.0 / 3.0
ratio_cap = 20.0


def neighbours(values):
    padded = jnp.pad(values, 1)
    return [padded[2:, 1:-1, 1:-1], padded[:-2, 1:-1, 1:-1], padded[1:-1, 2:, 1:-1], padded[1:-1, :-2, 1:-1], padded[1:-1, 1:-1, 2:], padded[1:-1, 1:-1, :-2]]


def summed(pieces):
    result = pieces[0] + pieces[1]
    for addend in pieces[2:]:
        result = result + addend
    return result


def diagonal_of(distance, fluid_cells):
    safe_dist = jnp.where(distance > 0, distance, 1.0)
    dist_near = neighbours(distance)
    fluid_near = neighbours(fluid_cells)
    term_list = [jnp.where(fluid_side > 0, 1.0, jnp.minimum((distance + dist_side) / safe_dist, ratio_cap)) for dist_side, fluid_side in zip(dist_near, fluid_near)]
    return jnp.where(fluid_cells > 0, summed(term_list), 1.0)


def operate(values, diagonal, fluid_cells):
    return fluid_cells * (diagonal * values - summed(neighbours(values)))


def smooth(residual, diagonal, fluid_cells, scale):
    first_pass = scale * residual
    second_pass = first_pass + scale * (residual - operate(first_pass, diagonal, fluid_cells))
    return second_pass, operate(second_pass, diagonal, fluid_cells)


def reference(divergence, level_set, tile_ids):
    listed = tile_ids.reshape(N_GX, N_GZ, SLOTS).astype(jnp.int32)
    device = lax.broadcasted_iota(jnp.int32, (N_GX, N_GZ, SLOTS), 0) * N_GZ + lax.broadcasted_iota(jnp.int32, (N_GX, N_GZ, SLOTS), 1)
    count_all = N_GX * N_GZ * TILES_DEV
    flat_ids = jnp.where(listed >= 0, device * TILES_DEV + listed, count_all).astype(jnp.int32)
    table = jnp.zeros((count_all + 1,), jnp.float32).at[flat_ids.reshape(-1)].set(1.0)[:count_all]
    table = table.reshape(N_GX, N_GZ, CX // TILE, CZ // TILE, NY // TILE).transpose(0, 2, 1, 3, 4)
    table = table.reshape(NX // TILE, NZ // TILE, NY // TILE)
    active = jnp.broadcast_to(table[:, None, :, None, :, None], (NX // TILE, TILE, NZ // TILE, TILE, NY // TILE, TILE)).reshape(NX, NZ, NY)
    fluid_cells = jnp.where(level_set < 0, active, 0.0)
    distance = jnp.abs(level_set)
    diagonal = diagonal_of(distance, fluid_cells)
    scale = damping / diagonal
    pressure = jnp.zeros_like(divergence)
    residual = fluid_cells * divergence
    smoothed, precond_image = smooth(residual, diagonal, fluid_cells, scale)
    gamma_now = jnp.sum(residual * smoothed)
    direction = smoothed
    operated = precond_image
    for iteration in range(ITERS):
        alpha_now = gamma_now / jnp.sum(direction * operated)
        pressure = pressure + alpha_now * direction
        residual = residual - alpha_now * operated
        if iteration + 1 < ITERS:
            smoothed, precond_image = smooth(residual, diagonal, fluid_cells, scale)
            gamma_next = jnp.sum(residual * smoothed)
            beta_now = gamma_next / gamma_now
            direction = smoothed + beta_now * direction
            operated = precond_image + beta_now * operated
            gamma_now = gamma_next
    return pressure, residual
```

```python
import functools

import jax
import jax.numpy as jnp
from jax import lax
from jax.experimental import pallas as pl
from jax.experimental.pallas import tpu as pltpu
from jax.sharding import PartitionSpec as P

MESH = pl.DeviceIdType.MESH
f32 = jnp.float32

CH, LANES = 4, 128
NX, NZ = 64, 16
X0, Z0 = 8, 5
PX, PZ = 80, 26
N_GX, N_GZ = 4, 32
SLOTS = 1024
SHIFT = 1.125
WALK = 9


def span(axis_len, origin, sign, near, far):
    if sign == 0:
        return origin, origin, axis_len
    if sign > 0:
        return origin + axis_len - far, origin - far, far - near + 1
    return origin - 1 + near, origin + axis_len - 1 + near, far - near + 1


def message_list():
    every = []
    for sx in (-1, 1):
        every.append(("ls", sx, 0, (1, 5), None, 0))
        every.append(("dv", sx, 0, (1, 4), None, 0))
    for sz in (-1, 1):
        every.append(("ls", 0, sz, None, (1, 3), 1))
        every.append(("dv", 0, sz, None, (1, 2), 1))
        every.append(("ls", 0, sz, None, (4, 5), 2))
        every.append(("dv", 0, sz, None, (3, 4), 2))
        for sx in (-1, 1):
            every.append(("ls", sx, sz, (1, 4), (1, 2), 1))
            every.append(("ls", sx, sz, (1, 2), (3, 4), 1))
            every.append(("dv", sx, sz, (1, 3), (1, 1), 1))
            every.append(("dv", sx, sz, (1, 2), (2, 3), 1))
    return every


MESSAGES = message_list()
AROUND = [(sx, sz) for sx in (-1, 0, 1) for sz in (-1, 0, 1)]


def main_kernel(
    dv_in, ls_in, ids_in,
    z0_ref, y_ref, r0_ref, w0_ref, u_ref, step_ref,
    ls, dv, air, gain, q1, q2, ids, table, sums, near_sum, far_sum,
    load_sem, send_sem, recv_sem, id_send, id_recv, ar_send, ar_recv,
):
    gx, gz = lax.axis_index("gx"), lax.axis_index("gz")
    core = lax.rem(gz, 2)
    place_z = lax.rem(gz // 2, 4)
    place_x = gz // 8

    def exists(sx, sz):
        ok = None
        for position, count, sign in ((gx, N_GX, sx), (gz, N_GZ, sz)):
            if sign:
                here = position < count - 1 if sign > 0 else position > 0
                ok = here if ok is None else jnp.logical_and(ok, here)
        return ok

    for number, (source, target) in enumerate(((ls_in, ls), (dv_in, dv))):
        for z in range(NZ):
            for c in range(CH):
                pltpu.make_async_copy(
                    source.at[:, z, pl.ds(c * LANES, LANES)],
                    target.at[c, Z0 + z, pl.ds(X0, NX)],
                    load_sem.at[number],
                ).start()
        if number == 0:
            own_ids = pltpu.make_async_copy(ids_in, ids.at[4], load_sem.at[2])
            own_ids.start()

    def own(array, number):
        region = array.at[:, pl.ds(Z0, NZ), pl.ds(X0, NX)]
        return pltpu.make_async_copy(region, region, load_sem.at[number])

    for k in range(9):
        if k != 4:
            ids[k] = jnp.full((1, SLOTS), -1, jnp.int32)

    def clear(z_first, z_count, x_first, x_count):
        def layer(z, carry):
            for array in (ls, dv):
                for c in range(CH):
                    array[c, z, pl.ds(x_first, x_count), :] = jnp.zeros((x_count, LANES), f32)
            return carry

        lax.fori_loop(z_first, z_first + z_count, layer, 0)

    pl.when(gx == 0)(lambda: clear(0, PZ, 0, X0))
    pl.when(gx == N_GX - 1)(lambda: clear(0, PZ, X0 + NX, 8))
    pl.when(gz == 0)(lambda: clear(0, Z0, 0, PX))
    pl.when(gz == N_GZ - 1)(lambda: clear(Z0 + NZ, 5, 0, PX))

    me_near = place_z * 2 + core
    me_far = gx * 4 + place_x

    def near_peer(i):
        return gx, place_x * 8 + (me_near ^ i)

    def far_peer(i):
        other = me_far ^ i
        return other // 4, lax.rem(other, 4) * 8 + me_near

    barrier = pltpu.get_barrier_semaphore()
    around = [(sx, sz) for sx, sz in AROUND if (sx, sz) != (0, 0)]
    for sx, sz in around:
        pl.when(exists(sx, sz))(
            lambda sx=sx, sz=sz: pl.semaphore_signal(
                barrier, inc=1, device_id=(gx + sx, gz + sz), device_id_type=MESH
            )
        )
    for i in range(1, 8):
        pl.semaphore_signal(barrier, inc=1, device_id=near_peer(i), device_id_type=MESH)
    for i in range(1, 16):
        pl.semaphore_signal(barrier, inc=1, device_id=far_peer(i), device_id_type=MESH)
    peers = 22
    for sx, sz in around:
        peers = peers + exists(sx, sz).astype(jnp.int32)
    pl.semaphore_wait(barrier, peers)

    def id_copy(sx, sz, peer=1):
        target = (1 - sx) * 3 + (1 - sz)
        return pltpu.make_async_remote_copy(
            ids.at[4], ids.at[target], id_send.at[target], id_recv.at[target],
            device_id=(gx + peer * sx, gz + peer * sz), device_id_type=MESH,
        )

    def layer_copy(number, peer=1):
        field, sx, sz, kx, kz, _ = MESSAGES[number]
        array = ls if field == "ls" else dv
        x_from, x_to, x_len = span(NX, X0, sx, *(kx or (0, 0)))
        z_from, z_to, z_len = span(NZ, Z0, sz, *(kz or (0, 0)))
        return pltpu.make_async_remote_copy(
            array.at[:, pl.ds(z_from, z_len), pl.ds(x_from, x_len)],
            array.at[:, pl.ds(z_to, z_len), pl.ds(x_to, x_len)],
            send_sem.at[number], recv_sem.at[number],
            device_id=(gx + peer * sx, gz + peer * sz), device_id_type=MESH,
        )

    def send(chosen):
        for number, message in enumerate(MESSAGES):
            if chosen(*message):
                _, sx, sz, _, _, _ = message
                pl.when(exists(sx, sz))(lambda number=number: layer_copy(number).start())

    def arrive(chosen):
        for number, message in enumerate(MESSAGES):
            if chosen(*message):
                _, sx, sz, _, _, _ = message
                pl.when(exists(-sx, -sz))(lambda number=number: layer_copy(number, -1).wait_recv())

    own_ids.wait()
    for sx, sz in around:
        pl.when(exists(sx, sz))(lambda sx=sx, sz=sz: id_copy(sx, sz).start())
    own(ls, 0).wait()
    send(lambda field, sx, sz, kx, kz, wave: field == "ls" and sx != 0 and sz == 0)
    send(lambda field, sx, sz, kx, kz, wave: field == "ls" and sx == 0 and wave == 1)
    send(lambda field, sx, sz, kx, kz, wave: field == "ls" and sx != 0 and sz != 0)
    own(dv, 1).wait()
    send(lambda field, sx, sz, kx, kz, wave: field == "dv" and sx == 0 and wave == 1)
    send(lambda field, sx, sz, kx, kz, wave: field == "dv" and sx != 0)
    send(lambda field, sx, sz, kx, kz, wave: wave == 2)

    row = lax.broadcasted_iota(jnp.int32, (40, 1), 0)
    row_z = (row >= 10).astype(jnp.int32) + (row >= 20).astype(jnp.int32) + (row >= 30).astype(jnp.int32)
    row_x = row - 10 * row_z
    from_device = (
        jnp.where(row_x == 0, 0, jnp.where(row_x == 9, 2, 1)) * 3
        + jnp.where(row_z == 0, 0, jnp.where(row_z == 3, 2, 1))
    )
    tile_x = jnp.where(row_x == 0, 7, jnp.where(row_x == 9, 0, row_x - 1))
    tile_z = jnp.where(row_z == 0, 1, jnp.where(row_z == 3, 0, row_z - 1))
    code = tile_x * 2 + tile_z
    for sx, sz in around:
        pl.when(exists(-sx, -sz))(lambda sx=sx, sz=sz: id_copy(sx, sz, -1).wait_recv())

    def listed(k, total):
        numbers = ids[k]
        wanted = jnp.where(from_device == k, code, -2)
        rows_hit = jnp.where((numbers >> 6) == wanted, 1.0, 0.0).astype(jnp.bfloat16)
        tile_y = lax.broadcasted_iota(jnp.int32, (64, 1), 0)
        y_hit = jnp.where((numbers & 63) == tile_y, 1.0, 0.0).astype(jnp.bfloat16)
        return total + lax.dot_general(
            rows_hit, y_hit, (((1,), (1,)), ((), ())), preferred_element_type=f32
        )

    tiles = lax.fori_loop(0, 9, listed, jnp.zeros((40, 64), f32))
    widen = lax.broadcasted_iota(jnp.int32, (64, CH * LANES), 1) >> 3
    widen = jnp.where(widen == lax.broadcasted_iota(jnp.int32, (64, CH * LANES), 0), 1.0, 0.0)
    cells = jnp.dot(tiles.astype(jnp.bfloat16), widen.astype(jnp.bfloat16), preferred_element_type=f32)
    for c in range(CH):
        table[c] = cells[:, c * LANES : (c + 1) * LANES]

    def layer_of(p):
        return jnp.where(core == 1, p, PZ - 1 - p)

    def flat(ref):
        return ref.reshape(CH, PZ * PX, LANES)

    ls_f, dv_f, air_f, gain_f, q1_f, q2_f, z0_f, y_f = map(
        flat, (ls, dv, air, gain, q1, q2, z0_ref, y_ref)
    )
    lane = lax.broadcasted_iota(jnp.int32, (8, LANES), 1)

    def rows_at(ref, r):
        return [ref[c, pl.ds(r, 8), :] for c in range(CH)]

    def beside(ref, r, middle):
        up = [pltpu.roll(v, LANES - 1, 1) for v in middle]
        down = [pltpu.roll(v, 1, 1) for v in middle]
        pieces = []
        for c in range(CH):
            after = up[c + 1] if c + 1 < CH else 0.0
            before = down[c - 1] if c > 0 else 0.0
            pieces.append(
                [
                    ref[c, pl.ds(r + 1, 8), :],
                    ref[c, pl.ds(r - 1, 8), :],
                    ref[c, pl.ds(r + PX, 8), :],
                    ref[c, pl.ds(r - PX, 8), :],
                    jnp.where(lane == LANES - 1, after, up[c]),
                    jnp.where(lane == 0, before, down[c]),
                ]
            )
        return pieces

    def added(parts):
        a, b, c, d, e, f = parts
        return ((a + b) + (c + d)) + (e + f)

    def walk(first, last, layer, carry=0):
        return lax.fori_loop(first, last + 1, lambda p, held: layer(layer_of(p), held), carry)

    def find_air(z, carry):
        base = z * PX
        row_of = 10 * (
            (z >= Z0).astype(jnp.int32) + (z >= Z0 + 8).astype(jnp.int32) + (z >= Z0 + 16).astype(jnp.int32)
        )
        for j in range(10):
            for c in range(CH):
                level = ls_f[c, pl.ds(base + 8 * j, 8), :]
                on = table[c, pl.ds(row_of + j, 1), :] > 0.5
                fluid = jnp.logical_and(level < 0, on)
                air_f[c, pl.ds(base + 8 * j, 8), :] = jnp.where(fluid, 0.0, jnp.abs(level))
        return carry

    def find_gain(z, carry):
        base = z * PX + 4
        for i in range(WALK):
            r = base + 8 * i
            middle = rows_at(air_f, r)
            level = rows_at(ls_f, r)
            value = rows_at(dv_f, r)
            for c, parts in enumerate(beside(air_f, r, middle)):
                distance = -level[c]
                most = 19.0 * distance
                extra = added([jnp.minimum(part, most) for part in parts])
                fluid = jnp.logical_and(middle[c] == 0.0, level[c] < 0)
                here = jnp.where(fluid, (2.0 / 3.0) * distance / (6.0 * distance + extra), 0.0)
                gain_f[c, pl.ds(r, 8), :] = here
                q1_f[c, pl.ds(r, 8), :] = here * value[c]
        return carry

    def stage(source, target, own_part, sign):
        def layer(z, carry):
            base = z * PX + 4
            for i in range(WALK):
                r = base + 8 * i
                middle = rows_at(source, r)
                for c, parts in enumerate(beside(source, r, middle)):
                    here = gain_f[c, pl.ds(r, 8), :] * added(parts)
                    target[c, pl.ds(r, 8), :] = own_part * middle[c] + sign * here
            return carry

        return layer

    find_z0 = stage(q1_f, z0_f, 4.0 / 3.0, 1.0)
    find_q2 = stage(z0_f, q2_f, 2.0 / 3.0, -1.0)
    find_y = stage(q2_f, y_f, 4.0 / 3.0, 1.0)

    def finish(z, held):
        base = z * PX + X0
        out = (z - Z0) * NX
        held = list(held)
        for i in range(NX // 8):
            r = base + 8 * i
            middle = rows_at(y_f, r)
            for c, parts in enumerate(beside(y_f, r, middle)):
                here = gain_f[c, pl.ds(r, 8), :]
                fluid = here > 0.0
                inverse = jnp.where(fluid, 1.0 / jnp.where(fluid, here, 1.0), 0.0)
                r0 = jnp.where(fluid, dv_f[c, pl.ds(r, 8), :], 0.0)
                w0 = inverse * q2_f[c, pl.ds(r, 8), :]
                u = inverse * ((2.0 / 3.0) * middle[c] - here * added(parts))
                z0 = z0_f[c, pl.ds(r, 8), :]
                y = middle[c]
                r0_ref[c, pl.ds(out + 8 * i, 8), :] = r0
                w0_ref[c, pl.ds(out + 8 * i, 8), :] = w0
                u_ref[c, pl.ds(out + 8 * i, 8), :] = u
                r_s, z_s, w_s = r0 - SHIFT * w0, z0 - SHIFT * y, w0 - SHIFT * u
                products = (r0 * z0, w0 * z0, r_s * z_s, w0 * z_s, w0 * y, w_s * z_s, w_s * y, u * y)
                held = [total + term for total, term in zip(held, products)]
        return tuple(held)

    from_above = lambda sz: sz == -1
    from_below = lambda sz: sz == 1
    for parity in (0, 1):
        early = from_above if parity == 0 else from_below

        @pl.when(core == parity)
        def _(early=early):
            arrive(lambda field, sx, sz, kx, kz, wave: sz != 0 and early(sz))

    arrive(lambda field, sx, sz, kx, kz, wave: sz == 0)
    walk(0, 20, find_air)
    walk(1, 19, find_gain)
    walk(2, 18, find_z0)
    walk(3, 17, find_q2)
    walk(4, 16, find_y)
    held = walk(5, 15, finish, tuple(jnp.zeros((8, LANES), f32) for _ in range(8)))

    for wave in (1, 2):
        for parity in (0, 1):
            late = from_below if parity == 0 else from_above

            @pl.when(core == parity)
            def _(late=late):
                arrive(lambda field, sx, sz, kx, kz, w: sz != 0 and w == wave and late(sz))

        if wave == 1:
            walk(21, 23, find_air)
            walk(20, 22, find_gain)
            walk(19, 21, find_z0)
            walk(18, 20, find_q2)
            walk(17, 19, find_y)
            held = walk(16, 18, finish, held)
        else:
            walk(24, 25, find_air)
            walk(23, 24, find_gain)
            walk(22, 23, find_z0)
            walk(21, 22, find_q2)
            walk(20, 21, find_y)
            held = walk(19, 20, finish, held)

    lane_row = lax.broadcasted_iota(jnp.int32, (1, LANES), 1)
    packed = jnp.zeros((1, LANES), f32)
    for k, total in enumerate(held):
        whole = jnp.sum(jnp.sum(total, axis=0, keepdims=True), axis=1, keepdims=True)
        packed = jnp.where(lane_row == k, whole, packed)

    def all_sum(value, buffer, count, peer, number):
        buffer[pl.ds(0, 1), :] = value
        for i in range(1, count):
            pltpu.make_async_remote_copy(
                buffer.at[pl.ds(0, 1)], buffer.at[pl.ds(i, 1)], ar_send.at[number], ar_recv.at[number],
                device_id=peer(i), device_id_type=MESH,
            ).start()
        every = pltpu.make_async_remote_copy(
            buffer.at[pl.ds(0, count - 1)], buffer.at[pl.ds(1, count - 1)], ar_send.at[number], ar_recv.at[number],
            device_id=peer(1), device_id_type=MESH,
        )
        every.wait_recv()
        result = jnp.sum(buffer[...], axis=0, keepdims=True)
        return result, every

    part, sent_near = all_sum(packed, near_sum, 8, near_peer, 0)
    whole, sent_far = all_sum(part, far_sum, 16, far_peer, 1)
    sums[pl.ds(0, 1), :] = whole
    gamma0, delta0, gamma_s, kappa, eta, delta_s, lam, theta = (
        sums[pl.ds(0, 1), pl.ds(k, 1)] for k in range(8)
    )
    alpha0 = gamma0 / delta0
    off = alpha0 - SHIFT
    gamma1 = gamma_s - 2.0 * off * kappa + off * off * eta
    delta1 = delta_s - 2.0 * off * lam + off * off * theta
    beta = gamma1 / gamma0
    below = delta1 - beta * gamma1 / alpha0
    alpha1 = jnp.where(below > 0, gamma1 / jnp.where(below > 0, below, 1.0), 0.0)
    for k, value in enumerate((alpha0, alpha1, beta)):
        step_ref[k] = jnp.broadcast_to(value, (8, LANES))

    for number, message in enumerate(MESSAGES):
        _, sx, sz, _, _, _ = message
        pl.when(exists(sx, sz))(lambda number=number: layer_copy(number).wait_send())
    for sx, sz in around:
        pl.when(exists(sx, sz))(lambda sx=sx, sz=sz: id_copy(sx, sz).wait_send())
    sent_near.wait_send()
    sent_far.wait_send()


def last_kernel(z0_ref, y_ref, r0_ref, w0_ref, u_ref, step_ref, p_out, r_out, p_buf, r_buf, sem):
    alpha0, alpha1, beta = step_ref[0], step_ref[1], step_ref[2]
    z0_f = z0_ref.reshape(CH, PZ * PX, LANES)
    y_f = y_ref.reshape(CH, PZ * PX, LANES)
    p_f = p_buf.reshape(CH, NZ * NX, LANES)
    r_f = r_buf.reshape(CH, NZ * NX, LANES)

    for z in range(NZ):
        def rows(i, carry, z=z):
            wide = (Z0 + z) * PX + X0 + 8 * i
            r = z * NX + 8 * i
            for c in range(CH):
                z0 = z0_f[c, pl.ds(wide, 8), :]
                z1 = z0 - alpha0 * y_f[c, pl.ds(wide, 8), :]
                p_f[c, pl.ds(r, 8), :] = alpha0 * z0 + alpha1 * (z1 + beta * z0)
                w0 = w0_ref[c, pl.ds(r, 8), :]
                w1 = w0 - alpha0 * u_ref[c, pl.ds(r, 8), :]
                r1 = r0_ref[c, pl.ds(r, 8), :] - alpha0 * w0
                r_f[c, pl.ds(r, 8), :] = r1 - alpha1 * (w1 + beta * w0)
            return carry

        lax.fori_loop(0, NX // 8, rows, 0, unroll=True)
        for number, (buffer, target) in enumerate(((p_buf, p_out), (r_buf, r_out))):
            for c in range(CH):
                pltpu.make_async_copy(
                    buffer.at[c, z], target.at[:, z, pl.ds(c * LANES, LANES)], sem.at[number]
                ).start()
    for number, buffer in enumerate((p_buf, r_buf)):
        pltpu.make_async_copy(buffer, buffer, sem.at[number]).wait()


def on_device(divergence, level_set, tile_ids):
    extended = (CH, PZ, PX, LANES)
    block = (CH, NZ * NX, LANES)
    held = pl.pallas_call(
        main_kernel,
        out_shape=[pltpu.VMEM(extended, f32)] * 2 + [pltpu.VMEM(block, f32)] * 3 + [pltpu.VMEM((3, 8, LANES), f32)],
        in_specs=[pl.BlockSpec(memory_space=pltpu.HBM)] * 3,
        out_specs=[pl.BlockSpec(memory_space=pltpu.VMEM)] * 6,
        scratch_shapes=[
            pltpu.VMEM(extended, f32), pltpu.VMEM(extended, f32), pltpu.VMEM(extended, f32),
            pltpu.VMEM(extended, f32), pltpu.VMEM(extended, f32), pltpu.VMEM(extended, f32),
            pltpu.VMEM((9, 1, SLOTS), jnp.int32),
            pltpu.VMEM((CH, 40, LANES), f32),
            pltpu.VMEM((8, LANES), f32),
            pltpu.VMEM((8, LANES), f32),
            pltpu.VMEM((16, LANES), f32),
            pltpu.SemaphoreType.DMA((3,)),
            pltpu.SemaphoreType.DMA((len(MESSAGES),)),
            pltpu.SemaphoreType.DMA((len(MESSAGES),)),
            pltpu.SemaphoreType.DMA((9,)),
            pltpu.SemaphoreType.DMA((9,)),
            pltpu.SemaphoreType.DMA((2,)),
            pltpu.SemaphoreType.DMA((2,)),
        ],
        compiler_params=pltpu.CompilerParams(
            collective_id=0, has_side_effects=True, vmem_limit_bytes=36 * 2**20
        ),
        name="solve",
    )(*(pltpu.with_memory_space_constraint(array, pltpu.HBM) for array in (divergence, level_set, tile_ids)))
    return pl.pallas_call(
        last_kernel,
        out_shape=[jax.ShapeDtypeStruct(divergence.shape, f32)] * 2,
        in_specs=[pl.BlockSpec(memory_space=pltpu.VMEM)] * 6,
        out_specs=[pl.BlockSpec(memory_space=pl.ANY)] * 2,
        scratch_shapes=[
            pltpu.VMEM((CH, NZ, NX, LANES), f32),
            pltpu.VMEM((CH, NZ, NX, LANES), f32),
            pltpu.SemaphoreType.DMA((2,)),
        ],
        compiler_params=pltpu.CompilerParams(vmem_limit_bytes=12 * 2**20),
        name="update",
    )(*held)


def solution(mesh):
    return jax.shard_map(
        on_device,
        mesh=mesh,
        in_specs=(P("gx", "gz", None), P("gx", "gz", None), P("gx", "gz")),
        out_specs=(P("gx", "gz", None), P("gx", "gz", None)),
        check_vma=False,
    )
```

```python
import functools

import jax
import jax.numpy as jnp
from jax import lax
from jax.experimental import pallas as pl
from jax.experimental.pallas import tpu as pltpu
from jax.sharding import PartitionSpec as P

MESH = pl.DeviceIdType.MESH
f32 = jnp.float32

CH, LANES = 4, 128
NX, NZ = 64, 16
X0, Z0 = 8, 5
PX, PZ = 80, 26
N_GX, N_GZ = 4, 32
SLOTS = 1024
SHIFT = 1.125
WALK = 9


def span(axis_len, origin, sign, near, far):
    if sign == 0:
        return origin, origin, axis_len
    if sign > 0:
        return origin + axis_len - far, origin - far, far - near + 1
    return origin - 1 + near, origin + axis_len - 1 + near, far - near + 1


def message_list():
    every = []
    for sx in (-1, 1):
        every.append(("ls", sx, 0, (1, 5), None, 0))
        every.append(("dv", sx, 0, (1, 4), None, 0))
    for sz in (-1, 1):
        every.append(("ls", 0, sz, None, (1, 3), 1))
        every.append(("dv", 0, sz, None, (1, 2), 1))
        every.append(("ls", 0, sz, None, (4, 5), 2))
        every.append(("dv", 0, sz, None, (3, 4), 2))
        for sx in (-1, 1):
            every.append(("ls", sx, sz, (1, 4), (1, 2), 1))
            every.append(("ls", sx, sz, (1, 2), (3, 4), 1))
            every.append(("dv", sx, sz, (1, 3), (1, 1), 1))
            every.append(("dv", sx, sz, (1, 2), (2, 3), 1))
    return every


MESSAGES = message_list()
AROUND = [(sx, sz) for sx in (-1, 0, 1) for sz in (-1, 0, 1)]


def main_kernel(
    dv_in, ls_in, ids_in,
    z0_ref, y_ref, r0_ref, w0_ref, u_ref, step_ref,
    ls, dv, air, gain, q1, q2, ids, table, sums, near_sum, far_sum,
    load_sem, send_sem, recv_sem, id_send, id_recv, ar_send, ar_recv,
):
    gx, gz = lax.axis_index("gx"), lax.axis_index("gz")
    core = lax.rem(gz, 2)
    place_z = lax.rem(gz // 2, 4)
    place_x = gz // 8

    def exists(sx, sz):
        ok = None
        for position, count, sign in ((gx, N_GX, sx), (gz, N_GZ, sz)):
            if sign:
                here = position < count - 1 if sign > 0 else position > 0
                ok = here if ok is None else jnp.logical_and(ok, here)
        return ok

    own_ids = pltpu.make_async_copy(ids_in, ids.at[4], load_sem.at[6])
    own_ids.start()
    parts = ((0, 5), (11, 5), (5, 6))
    for field, (source, target) in enumerate(((ls_in, ls), (dv_in, dv))):
        for part, (first, count) in enumerate(parts):
            for z in range(first, first + count):
                for c in range(CH):
                    pltpu.make_async_copy(
                        source.at[:, z, pl.ds(c * LANES, LANES)],
                        target.at[c, Z0 + z, pl.ds(X0, NX)],
                        load_sem.at[field * 3 + part],
                    ).start()

    def loaded(array, field, chosen):
        for part in chosen:
            first, count = parts[part]
            region = array.at[:, pl.ds(Z0 + first, count), pl.ds(X0, NX)]
            pltpu.make_async_copy(region, region, load_sem.at[field * 3 + part]).wait()

    for k in range(9):
        if k != 4:
            ids[k] = jnp.full((1, SLOTS), -1, jnp.int32)

    def clear(z_first, z_count, x_first, x_count):
        def layer(z, carry):
            for array in (ls, dv):
                for c in range(CH):
                    array[c, z, pl.ds(x_first, x_count), :] = jnp.zeros((x_count, LANES), f32)
            return carry

        lax.fori_loop(z_first, z_first + z_count, layer, 0)

    pl.when(gx == 0)(lambda: clear(0, PZ, 0, X0))
    pl.when(gx == N_GX - 1)(lambda: clear(0, PZ, X0 + NX, 8))
    pl.when(gz == 0)(lambda: clear(0, Z0, 0, PX))
    pl.when(gz == N_GZ - 1)(lambda: clear(Z0 + NZ, 5, 0, PX))

    me_near = place_z * 2 + core
    me_far = gx * 4 + place_x

    def near_peer(i):
        return gx, place_x * 8 + (me_near ^ i)

    def far_peer(i):
        other = me_far ^ i
        return other // 4, lax.rem(other, 4) * 8 + me_near

    barrier = pltpu.get_barrier_semaphore()
    around = [(sx, sz) for sx, sz in AROUND if (sx, sz) != (0, 0)]
    for sx, sz in around:
        pl.when(exists(sx, sz))(
            lambda sx=sx, sz=sz: pl.semaphore_signal(
                barrier, inc=1, device_id=(gx + sx, gz + sz), device_id_type=MESH
            )
        )
    for i in range(1, 8):
        pl.semaphore_signal(barrier, inc=1, device_id=near_peer(i), device_id_type=MESH)
    for i in range(1, 16):
        pl.semaphore_signal(barrier, inc=1, device_id=far_peer(i), device_id_type=MESH)
    peers = 22
    for sx, sz in around:
        peers = peers + exists(sx, sz).astype(jnp.int32)
    pl.semaphore_wait(barrier, peers)

    def id_copy(sx, sz, peer=1):
        target = (1 - sx) * 3 + (1 - sz)
        return pltpu.make_async_remote_copy(
            ids.at[4], ids.at[target], id_send.at[target], id_recv.at[target],
            device_id=(gx + peer * sx, gz + peer * sz), device_id_type=MESH,
        )

    def layer_copy(number, peer=1):
        field, sx, sz, kx, kz, _ = MESSAGES[number]
        array = ls if field == "ls" else dv
        x_from, x_to, x_len = span(NX, X0, sx, *(kx or (0, 0)))
        z_from, z_to, z_len = span(NZ, Z0, sz, *(kz or (0, 0)))
        return pltpu.make_async_remote_copy(
            array.at[:, pl.ds(z_from, z_len), pl.ds(x_from, x_len)],
            array.at[:, pl.ds(z_to, z_len), pl.ds(x_to, x_len)],
            send_sem.at[number], recv_sem.at[number],
            device_id=(gx + peer * sx, gz + peer * sz), device_id_type=MESH,
        )

    def send(chosen):
        for number, message in enumerate(MESSAGES):
            if chosen(*message):
                _, sx, sz, _, _, _ = message
                pl.when(exists(sx, sz))(lambda number=number: layer_copy(number).start())

    def arrive(chosen):
        for number, message in enumerate(MESSAGES):
            if chosen(*message):
                _, sx, sz, _, _, _ = message
                pl.when(exists(-sx, -sz))(lambda number=number: layer_copy(number, -1).wait_recv())

    own_ids.wait()
    for sx, sz in around:
        pl.when(exists(sx, sz))(lambda sx=sx, sz=sz: id_copy(sx, sz).start())
    loaded(ls, 0, (0, 1))
    send(lambda field, sx, sz, kx, kz, wave: field == "ls" and sx == 0 and wave == 1)
    loaded(ls, 0, (2,))
    send(lambda field, sx, sz, kx, kz, wave: field == "ls" and sx != 0 and sz == 0)
    send(lambda field, sx, sz, kx, kz, wave: field == "ls" and sx != 0 and sz != 0)
    loaded(dv, 1, (0, 1))
    send(lambda field, sx, sz, kx, kz, wave: field == "dv" and sx == 0 and wave == 1)
    loaded(dv, 1, (2,))
    send(lambda field, sx, sz, kx, kz, wave: field == "dv" and sx != 0 and sz == 0)
    send(lambda field, sx, sz, kx, kz, wave: field == "dv" and sx != 0 and sz != 0)
    send(lambda field, sx, sz, kx, kz, wave: wave == 2)

    row = lax.broadcasted_iota(jnp.int32, (40, 1), 0)
    row_z = (row >= 10).astype(jnp.int32) + (row >= 20).astype(jnp.int32) + (row >= 30).astype(jnp.int32)
    row_x = row - 10 * row_z
    from_device = (
        jnp.where(row_x == 0, 0, jnp.where(row_x == 9, 2, 1)) * 3
        + jnp.where(row_z == 0, 0, jnp.where(row_z == 3, 2, 1))
    )
    tile_x = jnp.where(row_x == 0, 7, jnp.where(row_x == 9, 0, row_x - 1))
    tile_z = jnp.where(row_z == 0, 1, jnp.where(row_z == 3, 0, row_z - 1))
    code = tile_x * 2 + tile_z

    def listed(k, total):
        numbers = ids[k]
        wanted = jnp.where(from_device == k, code, -2)
        rows_hit = jnp.where((numbers >> 6) == wanted, 1.0, 0.0).astype(jnp.bfloat16)
        tile_y = lax.broadcasted_iota(jnp.int32, (64, 1), 0)
        y_hit = jnp.where((numbers & 63) == tile_y, 1.0, 0.0).astype(jnp.bfloat16)
        return total + lax.dot_general(
            rows_hit, y_hit, (((1,), (1,)), ((), ())), preferred_element_type=f32
        )

    widen = lax.broadcasted_iota(jnp.int32, (64, CH * LANES), 1) >> 3
    widen = jnp.where(widen == lax.broadcasted_iota(jnp.int32, (64, CH * LANES), 0), 1.0, 0.0)
    widen = widen.astype(jnp.bfloat16)

    def fill_table(first, last):
        tiles = lax.fori_loop(first, last, listed, jnp.zeros((40, 64), f32))
        cells = jnp.dot(tiles.astype(jnp.bfloat16), widen, preferred_element_type=f32)
        for c in range(CH):
            table[c] = cells[:, c * LANES : (c + 1) * LANES]

    def layer_of(p):
        return jnp.where(core == 1, p, PZ - 1 - p)

    def flat(ref):
        return ref.reshape(CH, PZ * PX, LANES)

    ls_f, dv_f, air_f, gain_f, q1_f, q2_f, z0_f, y_f = map(
        flat, (ls, dv, air, gain, q1, q2, z0_ref, y_ref)
    )
    lane = lax.broadcasted_iota(jnp.int32, (8, LANES), 1)

    def rows_at(ref, r):
        return [ref[c, pl.ds(r, 8), :] for c in range(CH)]

    def beside(ref, r, middle):
        up = [pltpu.roll(v, LANES - 1, 1) for v in middle]
        down = [pltpu.roll(v, 1, 1) for v in middle]
        pieces = []
        for c in range(CH):
            after = up[c + 1] if c + 1 < CH else 0.0
            before = down[c - 1] if c > 0 else 0.0
            pieces.append(
                [
                    ref[c, pl.ds(r + 1, 8), :],
                    ref[c, pl.ds(r - 1, 8), :],
                    ref[c, pl.ds(r + PX, 8), :],
                    ref[c, pl.ds(r - PX, 8), :],
                    jnp.where(lane == LANES - 1, after, up[c]),
                    jnp.where(lane == 0, before, down[c]),
                ]
            )
        return pieces

    def added(parts):
        a, b, c, d, e, f = parts
        return ((a + b) + (c + d)) + (e + f)

    def walk(first, last, layer, held=0, group=3):
        rounds = (last - first + 1) // group

        def some(q, held):
            for step in range(group):
                held = layer(layer_of(first + q * group + step), held)
            return held

        if rounds > 1:
            held = lax.fori_loop(0, rounds, some, held)
            first = first + rounds * group
        for p in range(first, last + 1):
            held = layer(layer_of(p), held)
        return held

    def find_air(columns):
        def layer(z, carry):
            base = z * PX
            row_of = 10 * (
                (z >= Z0).astype(jnp.int32)
                + (z >= Z0 + 8).astype(jnp.int32)
                + (z >= Z0 + 16).astype(jnp.int32)
            )
            for j in columns:
                for c in range(CH):
                    level = ls_f[c, pl.ds(base + 8 * j, 8), :]
                    on = table[c, pl.ds(row_of + j, 1), :] > 0.5
                    fluid = jnp.logical_and(level < 0, on)
                    air_f[c, pl.ds(base + 8 * j, 8), :] = jnp.where(fluid, 0.0, jnp.abs(level))
            return carry

        return layer

    def find_gain(columns, with_q1=True):
        def layer(z, carry):
            base = z * PX + 4
            for i in columns:
                r = base + 8 * i
                middle = rows_at(air_f, r)
                for c, parts in enumerate(beside(air_f, r, middle)):
                    level = ls_f[c, pl.ds(r, 8), :]
                    distance = -level
                    most = 19.0 * distance
                    extra = added([jnp.minimum(part, most) for part in parts])
                    fluid = jnp.logical_and(middle[c] == 0.0, level < 0)
                    here = jnp.where(fluid, (2.0 / 3.0) * distance / (6.0 * distance + extra), 0.0)
                    gain_f[c, pl.ds(r, 8), :] = here
                    if with_q1:
                        q1_f[c, pl.ds(r, 8), :] = here * dv_f[c, pl.ds(r, 8), :]
            return carry

        return layer

    def find_q1(z, carry):
        for i in (0, WALK - 1):
            r = z * PX + 4 + 8 * i
            for c in range(CH):
                q1_f[c, pl.ds(r, 8), :] = gain_f[c, pl.ds(r, 8), :] * dv_f[c, pl.ds(r, 8), :]
        return carry

    def stage(source, target, own_part, sign):
        def layer(z, carry):
            base = z * PX + 4
            for i in range(WALK):
                r = base + 8 * i
                middle = rows_at(source, r)
                for c, parts in enumerate(beside(source, r, middle)):
                    here = gain_f[c, pl.ds(r, 8), :] * added(parts)
                    target[c, pl.ds(r, 8), :] = own_part * middle[c] + sign * here
            return carry

        return layer

    find_z0 = stage(q1_f, z0_f, 4.0 / 3.0, 1.0)
    find_q2 = stage(z0_f, q2_f, 2.0 / 3.0, -1.0)
    find_y = stage(q2_f, y_f, 4.0 / 3.0, 1.0)

    def finish(z, held):
        base = z * PX + X0
        out = (z - Z0) * NX
        held = list(held)
        for i in range(NX // 8):
            r = base + 8 * i
            middle = rows_at(y_f, r)
            for c, parts in enumerate(beside(y_f, r, middle)):
                here = gain_f[c, pl.ds(r, 8), :]
                fluid = here > 0.0
                inverse = jnp.where(fluid, 1.0 / jnp.where(fluid, here, 1.0), 0.0)
                r0 = jnp.where(fluid, dv_f[c, pl.ds(r, 8), :], 0.0)
                w0 = inverse * q2_f[c, pl.ds(r, 8), :]
                u = inverse * ((2.0 / 3.0) * middle[c] - here * added(parts))
                z0 = z0_f[c, pl.ds(r, 8), :]
                y = middle[c]
                r0_ref[c, pl.ds(out + 8 * i, 8), :] = r0
                w0_ref[c, pl.ds(out + 8 * i, 8), :] = w0
                u_ref[c, pl.ds(out + 8 * i, 8), :] = u
                r_s, z_s, w_s = r0 - SHIFT * w0, z0 - SHIFT * y, w0 - SHIFT * u
                products = (r0 * z0, w0 * z0, w0 * y, u * y, r_s * z_s, w_s * z_s)
                held = [total + term for total, term in zip(held, products)]
        return tuple(held)

    from_above = lambda sz: sz == -1
    from_below = lambda sz: sz == 1

    def arrive_at(side_of_even, side_of_odd, chosen):
        for parity, side in ((0, side_of_even), (1, side_of_odd)):

            @pl.when(core == parity)
            def _(side=side):
                arrive(lambda field, sx, sz, kx, kz, wave: side(sz) and chosen(field, sx, wave))

    def arrive_early(chosen):
        arrive_at(from_above, from_below, chosen)

    def arrive_late(chosen):
        arrive_at(from_below, from_above, chosen)

    every_column, inner = range(10), range(1, 9)
    edges, between = (0, WALK - 1), range(1, WALK - 1)
    fill_table(4, 5)
    walk(5, 20, find_air(inner))
    for sx, sz in around:
        pl.when(exists(-sx, -sz))(lambda sx=sx, sz=sz: id_copy(sx, sz, -1).wait_recv())
    fill_table(0, 9)
    arrive_early(lambda field, sx, wave: sx == 0)
    walk(0, 4, find_air(inner))
    walk(1, 19, find_gain(between))
    arrive(lambda field, sx, sz, kx, kz, wave: sz == 0 and field == "ls")
    arrive_early(lambda field, sx, wave: sx != 0 and field == "ls")
    walk(0, 20, find_air((0, 9)))
    walk(1, 19, find_gain(edges, False))
    arrive(lambda field, sx, sz, kx, kz, wave: sz == 0 and field == "dv")
    arrive_early(lambda field, sx, wave: sx != 0 and field == "dv")
    walk(1, 19, find_q1)
    walk(2, 18, find_z0)
    walk(3, 17, find_q2)
    walk(4, 16, find_y)
    held = walk(5, 15, finish, tuple(jnp.zeros((8, LANES), f32) for _ in range(6)))

    arrive_late(lambda field, sx, wave: wave == 1)
    walk(21, 23, find_air(every_column))
    walk(20, 22, find_gain(range(WALK)))
    walk(19, 21, find_z0)
    walk(18, 20, find_q2)
    walk(17, 19, find_y)
    held = walk(16, 18, finish, held)

    arrive_late(lambda field, sx, wave: wave == 2)
    walk(24, 25, find_air(every_column))
    walk(23, 24, find_gain(range(WALK)))
    walk(22, 23, find_z0)
    walk(21, 22, find_q2)
    walk(20, 21, find_y)
    held = walk(19, 20, finish, held)

    lane_row = lax.broadcasted_iota(jnp.int32, (1, LANES), 1)
    packed = jnp.zeros((1, LANES), f32)
    for k, total in enumerate(held):
        whole = jnp.sum(jnp.sum(total, axis=0, keepdims=True), axis=1, keepdims=True)
        packed = jnp.where(lane_row == k, whole, packed)

    def all_sum(value, buffer, count, peer, number):
        buffer[pl.ds(0, 1), :] = value
        for i in range(1, count):
            pltpu.make_async_remote_copy(
                buffer.at[pl.ds(0, 1)], buffer.at[pl.ds(i, 1)], ar_send.at[number], ar_recv.at[number],
                device_id=peer(i), device_id_type=MESH,
            ).start()
        every = pltpu.make_async_remote_copy(
            buffer.at[pl.ds(0, count - 1)], buffer.at[pl.ds(1, count - 1)], ar_send.at[number], ar_recv.at[number],
            device_id=peer(1), device_id_type=MESH,
        )
        every.wait_recv()
        result = jnp.sum(buffer[...], axis=0, keepdims=True)
        return result, every

    part, sent_near = all_sum(packed, near_sum, 8, near_peer, 0)
    whole, sent_far = all_sum(part, far_sum, 16, far_peer, 1)
    sums[pl.ds(0, 1), :] = whole
    gamma0, delta0, eta, theta, gamma_s, delta_s = (sums[pl.ds(0, 1), pl.ds(k, 1)] for k in range(6))
    alpha0 = gamma0 / delta0
    off = alpha0 - SHIFT
    kappa, lam = delta0 - SHIFT * eta, eta - SHIFT * theta
    gamma1 = gamma_s - 2.0 * off * kappa + off * off * eta
    delta1 = delta_s - 2.0 * off * lam + off * off * theta
    beta = gamma1 / gamma0
    below = delta1 - beta * gamma1 / alpha0
    alpha1 = jnp.where(below > 0, gamma1 / jnp.where(below > 0, below, 1.0), 0.0)
    for k, value in enumerate((alpha0, alpha1, beta)):
        step_ref[k] = jnp.broadcast_to(value, (8, LANES))

    for number, message in enumerate(MESSAGES):
        _, sx, sz, _, _, _ = message
        pl.when(exists(sx, sz))(lambda number=number: layer_copy(number).wait_send())
    for sx, sz in around:
        pl.when(exists(sx, sz))(lambda sx=sx, sz=sz: id_copy(sx, sz).wait_send())
    sent_near.wait_send()
    sent_far.wait_send()


def last_kernel(z0_ref, y_ref, r0_ref, w0_ref, u_ref, step_ref, p_out, r_out, p_buf, r_buf, sem):
    alpha0, alpha1, beta = step_ref[0], step_ref[1], step_ref[2]
    z0_f = z0_ref.reshape(CH, PZ * PX, LANES)
    y_f = y_ref.reshape(CH, PZ * PX, LANES)
    p_f = p_buf.reshape(CH, NZ * NX, LANES)
    r_f = r_buf.reshape(CH, NZ * NX, LANES)

    for z in range(NZ):
        def rows(i, carry, z=z):
            wide = (Z0 + z) * PX + X0 + 8 * i
            r = z * NX + 8 * i
            for c in range(CH):
                z0 = z0_f[c, pl.ds(wide, 8), :]
                z1 = z0 - alpha0 * y_f[c, pl.ds(wide, 8), :]
                p_f[c, pl.ds(r, 8), :] = alpha0 * z0 + alpha1 * (z1 + beta * z0)
                w0 = w0_ref[c, pl.ds(r, 8), :]
                w1 = w0 - alpha0 * u_ref[c, pl.ds(r, 8), :]
                r1 = r0_ref[c, pl.ds(r, 8), :] - alpha0 * w0
                r_f[c, pl.ds(r, 8), :] = r1 - alpha1 * (w1 + beta * w0)
            return carry

        lax.fori_loop(0, NX // 8, rows, 0, unroll=True)
        for number, (buffer, target) in enumerate(((p_buf, p_out), (r_buf, r_out))):
            for c in range(CH):
                pltpu.make_async_copy(
                    buffer.at[c, z], target.at[:, z, pl.ds(c * LANES, LANES)], sem.at[number]
                ).start()
    for number, buffer in enumerate((p_buf, r_buf)):
        pltpu.make_async_copy(buffer, buffer, sem.at[number]).wait()


def on_device(divergence, level_set, tile_ids):
    extended = (CH, PZ, PX, LANES)
    block = (CH, NZ * NX, LANES)
    held = pl.pallas_call(
        main_kernel,
        out_shape=[pltpu.VMEM(extended, f32)] * 2 + [pltpu.VMEM(block, f32)] * 3 + [pltpu.VMEM((3, 8, LANES), f32)],
        in_specs=[pl.BlockSpec(memory_space=pltpu.HBM)] * 3,
        out_specs=[pl.BlockSpec(memory_space=pltpu.VMEM)] * 6,
        scratch_shapes=[
            pltpu.VMEM(extended, f32), pltpu.VMEM(extended, f32), pltpu.VMEM(extended, f32),
            pltpu.VMEM(extended, f32), pltpu.VMEM(extended, f32), pltpu.VMEM(extended, f32),
            pltpu.VMEM((9, 1, SLOTS), jnp.int32),
            pltpu.VMEM((CH, 40, LANES), f32),
            pltpu.VMEM((8, LANES), f32),
            pltpu.VMEM((8, LANES), f32),
            pltpu.VMEM((16, LANES), f32),
            pltpu.SemaphoreType.DMA((7,)),
            pltpu.SemaphoreType.DMA((len(MESSAGES),)),
            pltpu.SemaphoreType.DMA((len(MESSAGES),)),
            pltpu.SemaphoreType.DMA((9,)),
            pltpu.SemaphoreType.DMA((9,)),
            pltpu.SemaphoreType.DMA((2,)),
            pltpu.SemaphoreType.DMA((2,)),
        ],
        compiler_params=pltpu.CompilerParams(
            collective_id=0, has_side_effects=True, vmem_limit_bytes=36 * 2**20
        ),
        name="solve",
    )(*(pltpu.with_memory_space_constraint(array, pltpu.HBM) for array in (divergence, level_set, tile_ids)))
    return pl.pallas_call(
        last_kernel,
        out_shape=[jax.ShapeDtypeStruct(divergence.shape, f32)] * 2,
        in_specs=[pl.BlockSpec(memory_space=pltpu.VMEM)] * 6,
        out_specs=[pl.BlockSpec(memory_space=pl.ANY)] * 2,
        scratch_shapes=[
            pltpu.VMEM((CH, NZ, NX, LANES), f32),
            pltpu.VMEM((CH, NZ, NX, LANES), f32),
            pltpu.SemaphoreType.DMA((2,)),
        ],
        compiler_params=pltpu.CompilerParams(vmem_limit_bytes=12 * 2**20),
        name="update",
    )(*held)


def solution(mesh):
    return jax.shard_map(
        on_device,
        mesh=mesh,
        in_specs=(P("gx", "gz", None), P("gx", "gz", None), P("gx", "gz")),
        out_specs=(P("gx", "gz", None), P("gx", "gz", None)),
        check_vma=False,
    )
```

```python
import functools

import jax
import jax.numpy as jnp
from jax import lax
from jax.experimental import pallas as pl
from jax.experimental.pallas import tpu as pltpu
from jax.sharding import PartitionSpec as P

MESH = pl.DeviceIdType.MESH
f32 = jnp.float32

CH, LANES = 4, 128
NX, NZ = 64, 16
X0, Z0 = 8, 5
PX, PZ = 80, 26
N_GX, N_GZ = 4, 32
SLOTS = 1024
SHIFT = 1.125
WALK = 9


def span(axis_len, origin, sign, near, far):
    if sign == 0:
        return origin, origin, axis_len
    if sign > 0:
        return origin + axis_len - far, origin - far, far - near + 1
    return origin - 1 + near, origin + axis_len - 1 + near, far - near + 1


def message_list():
    every = []
    for sx in (-1, 1):
        every.append(("ls", sx, 0, (1, 5), None, 0))
        every.append(("dv", sx, 0, (1, 4), None, 0))
    for sz in (-1, 1):
        every.append(("ls", 0, sz, None, (1, 4), 1))
        every.append(("dv", 0, sz, None, (1, 3), 1))
        every.append(("ls", 0, sz, None, (5, 5), 2))
        every.append(("dv", 0, sz, None, (4, 4), 2))
        for sx in (-1, 1):
            every.append(("ls", sx, sz, (1, 4), (1, 2), 1))
            every.append(("ls", sx, sz, (1, 2), (3, 4), 1))
            every.append(("dv", sx, sz, (1, 3), (1, 1), 1))
            every.append(("dv", sx, sz, (1, 2), (2, 3), 1))
    return every


MESSAGES = message_list()
AROUND = [(sx, sz) for sx in (-1, 0, 1) for sz in (-1, 0, 1)]


def main_kernel(
    dv_in, ls_in, ids_in,
    z0_ref, y_ref, r0_ref, w0_ref, u_ref, step_ref,
    ls, dv, air, dist, gain, q1, q2, ids, table, sums, near_sum, far_sum,
    load_sem, send_sem, recv_sem, id_send, id_recv, ar_send, ar_recv,
):
    gx, gz = lax.axis_index("gx"), lax.axis_index("gz")
    core = lax.rem(gz, 2)
    place_z = lax.rem(gz // 2, 4)
    place_x = gz // 8

    def exists(sx, sz):
        ok = None
        for position, count, sign in ((gx, N_GX, sx), (gz, N_GZ, sz)):
            if sign:
                here = position < count - 1 if sign > 0 else position > 0
                ok = here if ok is None else jnp.logical_and(ok, here)
        return ok

    for k in range(9):
        if k != 4:
            ids[k] = jnp.full((1, SLOTS), -1, jnp.int32)

    def clear(z_first, z_count, x_first, x_count):
        def layer(z, carry):
            for array in (ls, dv):
                for c in range(CH):
                    array[c, z, pl.ds(x_first, x_count), :] = jnp.zeros((x_count, LANES), f32)
            return carry

        lax.fori_loop(z_first, z_first + z_count, layer, 0)

    pl.when(gx == 0)(lambda: clear(0, PZ, 0, X0))
    pl.when(gx == N_GX - 1)(lambda: clear(0, PZ, X0 + NX, 8))
    pl.when(gz == 0)(lambda: clear(0, Z0, 0, PX))
    pl.when(gz == N_GZ - 1)(lambda: clear(Z0 + NZ, 5, 0, PX))

    me_near = place_z * 2 + core
    me_far = gx * 4 + place_x

    def near_peer(i):
        return gx, place_x * 8 + (me_near ^ i)

    def far_peer(i):
        other = me_far ^ i
        return other // 4, lax.rem(other, 4) * 8 + me_near

    barrier = pltpu.get_barrier_semaphore()
    around = [(sx, sz) for sx, sz in AROUND if (sx, sz) != (0, 0)]
    for sx, sz in around:
        pl.when(exists(sx, sz))(
            lambda sx=sx, sz=sz: pl.semaphore_signal(
                barrier, inc=1, device_id=(gx + sx, gz + sz), device_id_type=MESH
            )
        )
    for i in range(1, 8):
        pl.semaphore_signal(barrier, inc=1, device_id=near_peer(i), device_id_type=MESH)
    for i in range(1, 16):
        pl.semaphore_signal(barrier, inc=1, device_id=far_peer(i), device_id_type=MESH)
    own_ids = pltpu.make_async_copy(ids_in, ids.at[4], load_sem.at[6])
    own_ids.start()
    parts = ((0, 5), (11, 5), (5, 6))
    for field, (source, target) in enumerate(((ls_in, ls), (dv_in, dv))):
        for part, (first, count) in enumerate(parts):
            for z in range(first, first + count):
                for c in range(CH):
                    pltpu.make_async_copy(
                        source.at[:, z, pl.ds(c * LANES, LANES)],
                        target.at[c, Z0 + z, pl.ds(X0, NX)],
                        load_sem.at[field * 3 + part],
                    ).start()

    def loaded(array, field, chosen):
        for part in chosen:
            first, count = parts[part]
            region = array.at[:, pl.ds(Z0 + first, count), pl.ds(X0, NX)]
            pltpu.make_async_copy(region, region, load_sem.at[field * 3 + part]).wait()

    peers = 22
    for sx, sz in around:
        peers = peers + exists(sx, sz).astype(jnp.int32)
    pl.semaphore_wait(barrier, peers)

    def id_copy(sx, sz, peer=1):
        target = (1 - sx) * 3 + (1 - sz)
        return pltpu.make_async_remote_copy(
            ids.at[4], ids.at[target], id_send.at[target], id_recv.at[target],
            device_id=(gx + peer * sx, gz + peer * sz), device_id_type=MESH,
        )

    def layer_copy(number, peer=1):
        field, sx, sz, kx, kz, _ = MESSAGES[number]
        array = ls if field == "ls" else dv
        x_from, x_to, x_len = span(NX, X0, sx, *(kx or (0, 0)))
        z_from, z_to, z_len = span(NZ, Z0, sz, *(kz or (0, 0)))
        return pltpu.make_async_remote_copy(
            array.at[:, pl.ds(z_from, z_len), pl.ds(x_from, x_len)],
            array.at[:, pl.ds(z_to, z_len), pl.ds(x_to, x_len)],
            send_sem.at[number], recv_sem.at[number],
            device_id=(gx + peer * sx, gz + peer * sz), device_id_type=MESH,
        )

    def send(chosen):
        for number, message in enumerate(MESSAGES):
            if chosen(*message):
                _, sx, sz, _, _, _ = message
                pl.when(exists(sx, sz))(lambda number=number: layer_copy(number).start())

    def arrive(chosen):
        for number, message in enumerate(MESSAGES):
            if chosen(*message):
                _, sx, sz, _, _, _ = message
                pl.when(exists(-sx, -sz))(lambda number=number: layer_copy(number, -1).wait_recv())

    own_ids.wait()
    for sx, sz in around:
        pl.when(exists(sx, sz))(lambda sx=sx, sz=sz: id_copy(sx, sz).start())
    loaded(ls, 0, (0, 1))
    send(lambda field, sx, sz, kx, kz, wave: field == "ls" and sx == 0 and wave == 1)
    loaded(ls, 0, (2,))
    send(lambda field, sx, sz, kx, kz, wave: field == "ls" and sx != 0 and sz == 0)
    send(lambda field, sx, sz, kx, kz, wave: field == "ls" and sx != 0 and sz != 0)

    row = lax.broadcasted_iota(jnp.int32, (40, 1), 0)
    row_z = (row >= 10).astype(jnp.int32) + (row >= 20).astype(jnp.int32) + (row >= 30).astype(jnp.int32)
    row_x = row - 10 * row_z
    from_device = (
        jnp.where(row_x == 0, 0, jnp.where(row_x == 9, 2, 1)) * 3
        + jnp.where(row_z == 0, 0, jnp.where(row_z == 3, 2, 1))
    )
    tile_x = jnp.where(row_x == 0, 7, jnp.where(row_x == 9, 0, row_x - 1))
    tile_z = jnp.where(row_z == 0, 1, jnp.where(row_z == 3, 0, row_z - 1))
    code = tile_x * 2 + tile_z

    def listed(k, total):
        numbers = ids[k]
        wanted = jnp.where(from_device == k, code, -2)
        rows_hit = jnp.where((numbers >> 6) == wanted, 1.0, 0.0).astype(jnp.bfloat16)
        tile_y = lax.broadcasted_iota(jnp.int32, (64, 1), 0)
        y_hit = jnp.where((numbers & 63) == tile_y, 1.0, 0.0).astype(jnp.bfloat16)
        return total + lax.dot_general(
            rows_hit, y_hit, (((1,), (1,)), ((), ())), preferred_element_type=f32
        )

    widen = lax.broadcasted_iota(jnp.int32, (64, CH * LANES), 1) >> 3
    widen = jnp.where(widen == lax.broadcasted_iota(jnp.int32, (64, CH * LANES), 0), 1.0, 0.0)
    widen = widen.astype(jnp.bfloat16)

    def fill_table(first, last):
        tiles = lax.fori_loop(first, last, listed, jnp.zeros((40, 64), f32))
        cells = jnp.dot(tiles.astype(jnp.bfloat16), widen, preferred_element_type=f32)
        for c in range(CH):
            table[c] = cells[:, c * LANES : (c + 1) * LANES]

    def layer_of(p):
        return jnp.where(core == 1, p, PZ - 1 - p)

    def flat(ref):
        return ref.reshape(CH, PZ * PX, LANES)

    ls_f, dv_f, air_f, dist_f, gain_f, q1_f, q2_f, z0_f, y_f = map(
        flat, (ls, dv, air, dist, gain, q1, q2, z0_ref, y_ref)
    )
    lane = lax.broadcasted_iota(jnp.int32, (8, LANES), 1)

    def rows_at(ref, r):
        return [ref[c, pl.ds(r, 8), :] for c in range(CH)]

    def beside(ref, r, middle):
        up = [pltpu.roll(v, LANES - 1, 1) for v in middle]
        down = [pltpu.roll(v, 1, 1) for v in middle]
        pieces = []
        for c in range(CH):
            after = up[c + 1] if c + 1 < CH else 0.0
            before = down[c - 1] if c > 0 else 0.0
            pieces.append(
                [
                    ref[c, pl.ds(r + 1, 8), :],
                    ref[c, pl.ds(r - 1, 8), :],
                    ref[c, pl.ds(r + PX, 8), :],
                    ref[c, pl.ds(r - PX, 8), :],
                    jnp.where(lane == LANES - 1, after, up[c]),
                    jnp.where(lane == 0, before, down[c]),
                ]
            )
        return pieces

    def added(parts):
        a, b, c, d, e, f = parts
        return ((a + b) + (c + d)) + (e + f)

    def walk(first, last, layer, held=0, group=3):
        rounds = (last - first + 1) // group

        def some(q, held):
            for step in range(group):
                held = layer(layer_of(first + q * group + step), held)
            return held

        if rounds > 1:
            held = lax.fori_loop(0, rounds, some, held)
            first = first + rounds * group
        for p in range(first, last + 1):
            held = layer(layer_of(p), held)
        return held

    def find_air(columns):
        def layer(z, carry):
            base = z * PX
            row_of = 10 * (
                (z >= Z0).astype(jnp.int32)
                + (z >= Z0 + 8).astype(jnp.int32)
                + (z >= Z0 + 16).astype(jnp.int32)
            )
            for j in columns:
                for c in range(CH):
                    level = ls_f[c, pl.ds(base + 8 * j, 8), :]
                    on = table[c, pl.ds(row_of + j, 1), :] > 0.5
                    fluid = jnp.logical_and(level < 0, on)
                    air_f[c, pl.ds(base + 8 * j, 8), :] = jnp.where(fluid, 0.0, jnp.abs(level))
                    dist_f[c, pl.ds(base + 8 * j, 8), :] = jnp.where(fluid, -level, 0.0)
            return carry

        return layer

    def find_gain(columns, with_q1=True):
        def layer(z, carry):
            base = z * PX + 4
            for i in columns:
                r = base + 8 * i
                middle = rows_at(air_f, r)
                for c, parts in enumerate(beside(air_f, r, middle)):
                    distance = dist_f[c, pl.ds(r, 8), :]
                    most = 19.0 * distance
                    extra = added([jnp.minimum(part, most) for part in parts])
                    below = jnp.maximum(6.0 * distance + extra, 0.1)
                    here = (2.0 / 3.0) * distance / below
                    gain_f[c, pl.ds(r, 8), :] = here
                    if with_q1:
                        q1_f[c, pl.ds(r, 8), :] = here * dv_f[c, pl.ds(r, 8), :]
            return carry

        return layer

    def find_q1(z, carry):
        for i in (0, WALK - 1):
            r = z * PX + 4 + 8 * i
            for c in range(CH):
                q1_f[c, pl.ds(r, 8), :] = gain_f[c, pl.ds(r, 8), :] * dv_f[c, pl.ds(r, 8), :]
        return carry

    def stage(source, target, own_part, sign, columns=range(WALK)):
        def layer(z, carry):
            base = z * PX + 4
            for i in columns:
                r = base + 8 * i
                middle = rows_at(source, r)
                for c, parts in enumerate(beside(source, r, middle)):
                    here = gain_f[c, pl.ds(r, 8), :] * added(parts)
                    target[c, pl.ds(r, 8), :] = own_part * middle[c] + sign * here
            return carry

        return layer

    def find_z0(columns=range(WALK)):
        return stage(q1_f, z0_f, 4.0 / 3.0, 1.0, columns)

    def find_q2(columns=range(WALK)):
        return stage(z0_f, q2_f, 2.0 / 3.0, -1.0, columns)

    find_y = stage(q2_f, y_f, 4.0 / 3.0, 1.0)

    def finish(z, held):
        base = z * PX + X0
        out = (z - Z0) * NX
        held = list(held)
        for i in range(NX // 8):
            r = base + 8 * i
            middle = rows_at(y_f, r)
            for c, parts in enumerate(beside(y_f, r, middle)):
                here = gain_f[c, pl.ds(r, 8), :]
                inverse = 1.0 / jnp.maximum(here, 1e-3)
                r0 = jnp.where(here > 0.0, dv_f[c, pl.ds(r, 8), :], 0.0)
                w0 = inverse * q2_f[c, pl.ds(r, 8), :]
                u = inverse * ((2.0 / 3.0) * middle[c] - here * added(parts))
                z0 = z0_f[c, pl.ds(r, 8), :]
                y = middle[c]
                r0_ref[c, pl.ds(out + 8 * i, 8), :] = r0
                w0_ref[c, pl.ds(out + 8 * i, 8), :] = w0
                u_ref[c, pl.ds(out + 8 * i, 8), :] = u
                r_s, z_s, w_s = r0 - SHIFT * w0, z0 - SHIFT * y, w0 - SHIFT * u
                products = (r0 * z0, w0 * z0, w0 * y, u * y, r_s * z_s, w_s * z_s)
                held = [total + term for total, term in zip(held, products)]
        return tuple(held)

    from_above = lambda sz: sz == -1
    from_below = lambda sz: sz == 1

    def arrive_at(side_of_even, side_of_odd, chosen):
        for parity, side in ((0, side_of_even), (1, side_of_odd)):

            @pl.when(core == parity)
            def _(side=side):
                arrive(lambda field, sx, sz, kx, kz, wave: side(sz) and chosen(field, sx, wave))

    def arrive_early(chosen):
        arrive_at(from_above, from_below, chosen)

    def arrive_late(chosen):
        arrive_at(from_below, from_above, chosen)

    every_column, inner = range(10), range(1, 9)
    edges, between = (0, WALK - 1), range(1, WALK - 1)
    fill_table(4, 5)
    walk(5, 20, find_air(inner))
    loaded(dv, 1, (0, 1))
    send(lambda field, sx, sz, kx, kz, wave: field == "dv" and sx == 0 and wave == 1)
    loaded(dv, 1, (2,))
    send(lambda field, sx, sz, kx, kz, wave: field == "dv" and sx != 0 and sz == 0)
    send(lambda field, sx, sz, kx, kz, wave: field == "dv" and sx != 0 and sz != 0)
    send(lambda field, sx, sz, kx, kz, wave: wave == 2)
    walk(6, 19, find_gain(between))
    for sx, sz in around:
        pl.when(exists(-sx, -sz))(lambda sx=sx, sz=sz: id_copy(sx, sz, -1).wait_recv())
    fill_table(0, 9)
    arrive_early(lambda field, sx, wave: sx == 0)
    walk(0, 4, find_air(inner))
    walk(1, 5, find_gain(between))
    arrive(lambda field, sx, sz, kx, kz, wave: sz == 0 and field == "ls")
    arrive_early(lambda field, sx, wave: sx != 0 and field == "ls")
    walk(0, 20, find_air((0, 9)))
    walk(1, 19, find_gain(edges, False))
    walk(2, 18, find_z0(range(2, 7)))
    walk(3, 17, find_q2(range(3, 6)), group=5)
    arrive(lambda field, sx, sz, kx, kz, wave: sz == 0 and field == "dv")
    arrive_early(lambda field, sx, wave: sx != 0 and field == "dv")
    walk(1, 19, find_q1)
    walk(2, 18, find_z0((0, 1, 7, 8)), group=4)
    walk(3, 17, find_q2((0, 1, 2, 6, 7, 8)))
    walk(4, 16, find_y)
    held = walk(5, 15, finish, tuple(jnp.zeros((8, LANES), f32) for _ in range(6)))

    arrive_late(lambda field, sx, wave: wave == 1)
    walk(21, 24, find_air(every_column), group=2)
    walk(20, 23, find_gain(range(WALK)), group=2)
    walk(19, 22, find_z0(), group=2)
    walk(18, 21, find_q2(), group=2)
    walk(17, 20, find_y, group=2)
    held = walk(16, 19, finish, held, group=2)

    arrive_late(lambda field, sx, wave: wave == 2)
    walk(25, 25, find_air(every_column))
    walk(24, 24, find_gain(range(WALK)))
    walk(23, 23, find_z0())
    walk(22, 22, find_q2())
    walk(21, 21, find_y)
    held = walk(20, 20, finish, held)

    lane_row = lax.broadcasted_iota(jnp.int32, (1, LANES), 1)
    packed = jnp.zeros((1, LANES), f32)
    for k, total in enumerate(held):
        whole = jnp.sum(jnp.sum(total, axis=0, keepdims=True), axis=1, keepdims=True)
        packed = jnp.where(lane_row == k, whole, packed)

    def all_sum(value, buffer, count, peer, number):
        buffer[pl.ds(0, 1), :] = value
        for i in range(1, count):
            pltpu.make_async_remote_copy(
                buffer.at[pl.ds(0, 1)], buffer.at[pl.ds(i, 1)], ar_send.at[number], ar_recv.at[number],
                device_id=peer(i), device_id_type=MESH,
            ).start()
        every = pltpu.make_async_remote_copy(
            buffer.at[pl.ds(0, count - 1)], buffer.at[pl.ds(1, count - 1)], ar_send.at[number], ar_recv.at[number],
            device_id=peer(1), device_id_type=MESH,
        )
        every.wait_recv()
        result = jnp.sum(buffer[...], axis=0, keepdims=True)
        return result, every

    part, sent_near = all_sum(packed, near_sum, 8, near_peer, 0)
    whole, sent_far = all_sum(part, far_sum, 16, far_peer, 1)
    sums[pl.ds(0, 1), :] = whole
    gamma0, delta0, eta, theta, gamma_s, delta_s = (sums[pl.ds(0, 1), pl.ds(k, 1)] for k in range(6))
    alpha0 = gamma0 / delta0
    off = alpha0 - SHIFT
    kappa, lam = delta0 - SHIFT * eta, eta - SHIFT * theta
    gamma1 = gamma_s - 2.0 * off * kappa + off * off * eta
    delta1 = delta_s - 2.0 * off * lam + off * off * theta
    beta = gamma1 / gamma0
    below = delta1 - beta * gamma1 / alpha0
    alpha1 = jnp.where(below > 0, gamma1 / jnp.where(below > 0, below, 1.0), 0.0)
    for k, value in enumerate((alpha0, alpha1, beta)):
        step_ref[k] = jnp.broadcast_to(value, (8, LANES))

    for number, message in enumerate(MESSAGES):
        _, sx, sz, _, _, _ = message
        pl.when(exists(sx, sz))(lambda number=number: layer_copy(number).wait_send())
    for sx, sz in around:
        pl.when(exists(sx, sz))(lambda sx=sx, sz=sz: id_copy(sx, sz).wait_send())
    sent_near.wait_send()
    sent_far.wait_send()


def last_kernel(z0_ref, y_ref, r0_ref, w0_ref, u_ref, step_ref, p_out, r_out, p_buf, r_buf, sem):
    alpha0, alpha1, beta = step_ref[0], step_ref[1], step_ref[2]
    z0_f = z0_ref.reshape(CH, PZ * PX, LANES)
    y_f = y_ref.reshape(CH, PZ * PX, LANES)
    p_f = p_buf.reshape(CH, NZ * NX, LANES)
    r_f = r_buf.reshape(CH, NZ * NX, LANES)

    for z in range(NZ):
        def rows(i, carry, z=z):
            wide = (Z0 + z) * PX + X0 + 8 * i
            r = z * NX + 8 * i
            for c in range(CH):
                z0 = z0_f[c, pl.ds(wide, 8), :]
                z1 = z0 - alpha0 * y_f[c, pl.ds(wide, 8), :]
                p_f[c, pl.ds(r, 8), :] = alpha0 * z0 + alpha1 * (z1 + beta * z0)
                w0 = w0_ref[c, pl.ds(r, 8), :]
                w1 = w0 - alpha0 * u_ref[c, pl.ds(r, 8), :]
                r1 = r0_ref[c, pl.ds(r, 8), :] - alpha0 * w0
                r_f[c, pl.ds(r, 8), :] = r1 - alpha1 * (w1 + beta * w0)
            return carry

        lax.fori_loop(0, NX // 8, rows, 0, unroll=True)
        for number, (buffer, target) in enumerate(((p_buf, p_out), (r_buf, r_out))):
            for c in range(CH):
                pltpu.make_async_copy(
                    buffer.at[c, z], target.at[:, z, pl.ds(c * LANES, LANES)], sem.at[number]
                ).start()
    for number, buffer in enumerate((p_buf, r_buf)):
        pltpu.make_async_copy(buffer, buffer, sem.at[number]).wait()


def on_device(divergence, level_set, tile_ids):
    extended = (CH, PZ, PX, LANES)
    block = (CH, NZ * NX, LANES)
    held = pl.pallas_call(
        main_kernel,
        out_shape=[pltpu.VMEM(extended, f32)] * 2 + [pltpu.VMEM(block, f32)] * 3 + [pltpu.VMEM((3, 8, LANES), f32)],
        in_specs=[pl.BlockSpec(memory_space=pltpu.HBM)] * 3,
        out_specs=[pl.BlockSpec(memory_space=pltpu.VMEM)] * 6,
        scratch_shapes=[
            *[pltpu.VMEM(extended, f32)] * 7,
            pltpu.VMEM((9, 1, SLOTS), jnp.int32),
            pltpu.VMEM((CH, 40, LANES), f32),
            pltpu.VMEM((8, LANES), f32),
            pltpu.VMEM((8, LANES), f32),
            pltpu.VMEM((16, LANES), f32),
            pltpu.SemaphoreType.DMA((7,)),
            pltpu.SemaphoreType.DMA((len(MESSAGES),)),
            pltpu.SemaphoreType.DMA((len(MESSAGES),)),
            pltpu.SemaphoreType.DMA((9,)),
            pltpu.SemaphoreType.DMA((9,)),
            pltpu.SemaphoreType.DMA((2,)),
            pltpu.SemaphoreType.DMA((2,)),
        ],
        compiler_params=pltpu.CompilerParams(
            collective_id=0, has_side_effects=True, vmem_limit_bytes=40 * 2**20
        ),
        name="solve",
    )(*(pltpu.with_memory_space_constraint(array, pltpu.HBM) for array in (divergence, level_set, tile_ids)))
    return pl.pallas_call(
        last_kernel,
        out_shape=[jax.ShapeDtypeStruct(divergence.shape, f32)] * 2,
        in_specs=[pl.BlockSpec(memory_space=pltpu.VMEM)] * 6,
        out_specs=[pl.BlockSpec(memory_space=pl.ANY)] * 2,
        scratch_shapes=[
            pltpu.VMEM((CH, NZ, NX, LANES), f32),
            pltpu.VMEM((CH, NZ, NX, LANES), f32),
            pltpu.SemaphoreType.DMA((2,)),
        ],
        compiler_params=pltpu.CompilerParams(vmem_limit_bytes=12 * 2**20),
        name="update",
    )(*held)


def solution(mesh):
    return jax.shard_map(
        on_device,
        mesh=mesh,
        in_specs=(P("gx", "gz", None), P("gx", "gz", None), P("gx", "gz")),
        out_specs=(P("gx", "gz", None), P("gx", "gz", None)),
        check_vma=False,
    )
```

```python
import functools

import jax
import jax.numpy as jnp
from jax import lax
from jax.experimental import pallas as pl
from jax.experimental.pallas import tpu as pltpu
from jax.sharding import PartitionSpec as P

MESH = pl.DeviceIdType.MESH
f32 = jnp.float32

CH, LANES = 4, 128
NX, NZ = 64, 16
X0, Z0 = 8, 5
PX, PZ = 80, 26
N_GX, N_GZ = 4, 32
DEVICES = N_GX * N_GZ
SLOTS = 1024
SHIFT = 1.125
WALK = 9


def span(axis_len, origin, sign, near, far):
    if sign == 0:
        return origin, origin, axis_len
    if sign > 0:
        return origin + axis_len - far, origin - far, far - near + 1
    return origin - 1 + near, origin + axis_len - 1 + near, far - near + 1


def message_list():
    every = []
    for sx in (-1, 1):
        every.append(("ls", sx, 0, (1, 5), None, 0))
        every.append(("dv", sx, 0, (1, 4), None, 0))
    for sz in (-1, 1):
        every.append(("ls", 0, sz, None, (1, 4), 1))
        every.append(("dv", 0, sz, None, (1, 3), 1))
        every.append(("ls", 0, sz, None, (5, 5), 2))
        every.append(("dv", 0, sz, None, (4, 4), 2))
        for sx in (-1, 1):
            every.append(("ls", sx, sz, (1, 4), (1, 2), 1))
            every.append(("ls", sx, sz, (1, 2), (3, 4), 1))
            every.append(("dv", sx, sz, (1, 3), (1, 1), 1))
            every.append(("dv", sx, sz, (1, 2), (2, 3), 1))
    return every


MESSAGES = message_list()
AROUND = [(sx, sz) for sx in (-1, 0, 1) for sz in (-1, 0, 1)]


def main_kernel(
    dv_in, ls_in, ids_in,
    z0_ref, y_ref, r0_ref, w0_ref, u_ref, step_ref,
    ls, dv, air, dist, gain, q1, q2, ids, table, sums, every_sum,
    load_sem, send_sem, recv_sem, id_send, id_recv, ar_send, ar_recv, word_sem,
):
    gx, gz = lax.axis_index("gx"), lax.axis_index("gz")
    core = lax.rem(gz, 2)
    place_z = lax.rem(gz // 2, 4)
    place_x = gz // 8

    def exists(sx, sz):
        ok = None
        for position, count, sign in ((gx, N_GX, sx), (gz, N_GZ, sz)):
            if sign:
                here = position < count - 1 if sign > 0 else position > 0
                ok = here if ok is None else jnp.logical_and(ok, here)
        return ok

    for k in range(9):
        if k != 4:
            ids[k] = jnp.full((1, SLOTS), -1, jnp.int32)

    def clear(z_first, z_count, x_first, x_count):
        def layer(z, carry):
            for array in (ls, dv):
                for c in range(CH):
                    array[c, z, pl.ds(x_first, x_count), :] = jnp.zeros((x_count, LANES), f32)
            return carry

        lax.fori_loop(z_first, z_first + z_count, layer, 0)

    pl.when(gx == 0)(lambda: clear(0, PZ, 0, X0))
    pl.when(gx == N_GX - 1)(lambda: clear(0, PZ, X0 + NX, 8))
    pl.when(gz == 0)(lambda: clear(0, Z0, 0, PX))
    pl.when(gz == N_GZ - 1)(lambda: clear(Z0 + NZ, 5, 0, PX))

    me_chip = (gx * 4 + place_x) * 4 + place_z

    def sum_peer(i):
        chip = me_chip ^ (i >> 1)
        return chip // 16, lax.rem(chip, 16) * 2 + (core ^ (i & 1))

    barrier = pltpu.get_barrier_semaphore()
    around = [(sx, sz) for sx, sz in AROUND if (sx, sz) != (0, 0)]
    for sx, sz in around:
        pl.when(exists(sx, sz))(
            lambda sx=sx, sz=sz: pl.semaphore_signal(
                barrier, inc=1, device_id=(gx + sx, gz + sz), device_id_type=MESH
            )
        )
    own_ids = pltpu.make_async_copy(ids_in, ids.at[4], load_sem.at[6])
    own_ids.start()
    parts = ((0, 5), (11, 5), (5, 6))
    for field, (source, target) in enumerate(((ls_in, ls), (dv_in, dv))):
        for part, (first, count) in enumerate(parts):
            for z in range(first, first + count):
                for c in range(CH):
                    pltpu.make_async_copy(
                        source.at[:, z, pl.ds(c * LANES, LANES)],
                        target.at[c, Z0 + z, pl.ds(X0, NX)],
                        load_sem.at[field * 3 + part],
                    ).start()

    def loaded(array, field, chosen):
        for part in chosen:
            first, count = parts[part]
            region = array.at[:, pl.ds(Z0 + first, count), pl.ds(X0, NX)]
            pltpu.make_async_copy(region, region, load_sem.at[field * 3 + part]).wait()

    peers = 0
    for sx, sz in around:
        peers = peers + exists(sx, sz).astype(jnp.int32)
    pl.semaphore_wait(barrier, peers)

    reach = [(0, 1), (0, 2), (0, 4), (0, 8), (0, 16), (1, 0), (2, 0)]

    def greeted(step):
        dx, dz = reach[step]
        for sign in (-1, 1):
            if dx:
                ok = gx + dx < N_GX if sign > 0 else gx >= dx
            else:
                ok = gz + dz < N_GZ if sign > 0 else gz >= dz
            yield ok, (gx + sign * dx, gz + sign * dz)

    def greet(step):
        for ok, peer in greeted(step):
            pl.when(ok)(
                lambda peer=peer: pl.semaphore_signal(
                    word_sem.at[step], inc=1, device_id=peer, device_id_type=MESH
                )
            )

    def heed(step):
        count = 0
        for ok, _ in greeted(step):
            count = count + ok.astype(jnp.int32)
        pl.semaphore_wait(word_sem.at[step], count)
        if step + 1 < len(reach):
            greet(step + 1)

    greet(0)

    def id_copy(sx, sz, peer=1):
        target = (1 - sx) * 3 + (1 - sz)
        return pltpu.make_async_remote_copy(
            ids.at[4], ids.at[target], id_send.at[target], id_recv.at[target],
            device_id=(gx + peer * sx, gz + peer * sz), device_id_type=MESH,
        )

    def layer_copy(number, peer=1):
        field, sx, sz, kx, kz, _ = MESSAGES[number]
        array = ls if field == "ls" else dv
        x_from, x_to, x_len = span(NX, X0, sx, *(kx or (0, 0)))
        z_from, z_to, z_len = span(NZ, Z0, sz, *(kz or (0, 0)))
        return pltpu.make_async_remote_copy(
            array.at[:, pl.ds(z_from, z_len), pl.ds(x_from, x_len)],
            array.at[:, pl.ds(z_to, z_len), pl.ds(x_to, x_len)],
            send_sem.at[number], recv_sem.at[number],
            device_id=(gx + peer * sx, gz + peer * sz), device_id_type=MESH,
        )

    def send(chosen):
        for number, message in enumerate(MESSAGES):
            if chosen(*message):
                _, sx, sz, _, _, _ = message
                pl.when(exists(sx, sz))(lambda number=number: layer_copy(number).start())

    def arrive(chosen):
        for number, message in enumerate(MESSAGES):
            if chosen(*message):
                _, sx, sz, _, _, _ = message
                pl.when(exists(-sx, -sz))(lambda number=number: layer_copy(number, -1).wait_recv())

    own_ids.wait()
    for sx, sz in around:
        pl.when(exists(sx, sz))(lambda sx=sx, sz=sz: id_copy(sx, sz).start())
    loaded(ls, 0, (0, 1))
    send(lambda field, sx, sz, kx, kz, wave: field == "ls" and sx == 0 and wave == 1)
    loaded(ls, 0, (2,))
    send(lambda field, sx, sz, kx, kz, wave: field == "ls" and sx != 0 and sz == 0)
    send(lambda field, sx, sz, kx, kz, wave: field == "ls" and sx != 0 and sz != 0)

    row = lax.broadcasted_iota(jnp.int32, (40, 1), 0)
    row_z = (row >= 10).astype(jnp.int32) + (row >= 20).astype(jnp.int32) + (row >= 30).astype(jnp.int32)
    row_x = row - 10 * row_z
    from_device = (
        jnp.where(row_x == 0, 0, jnp.where(row_x == 9, 2, 1)) * 3
        + jnp.where(row_z == 0, 0, jnp.where(row_z == 3, 2, 1))
    )
    tile_x = jnp.where(row_x == 0, 7, jnp.where(row_x == 9, 0, row_x - 1))
    tile_z = jnp.where(row_z == 0, 1, jnp.where(row_z == 3, 0, row_z - 1))
    code = tile_x * 2 + tile_z

    def listed(k, total):
        numbers = ids[k]
        wanted = jnp.where(from_device == k, code, -2)
        rows_hit = jnp.where((numbers >> 6) == wanted, 1.0, 0.0).astype(jnp.bfloat16)
        tile_y = lax.broadcasted_iota(jnp.int32, (64, 1), 0)
        y_hit = jnp.where((numbers & 63) == tile_y, 1.0, 0.0).astype(jnp.bfloat16)
        return total + lax.dot_general(
            rows_hit, y_hit, (((1,), (1,)), ((), ())), preferred_element_type=f32
        )

    widen = lax.broadcasted_iota(jnp.int32, (64, CH * LANES), 1) >> 3
    widen = jnp.where(widen == lax.broadcasted_iota(jnp.int32, (64, CH * LANES), 0), 1.0, 0.0)
    widen = widen.astype(jnp.bfloat16)

    def fill_table(first, last):
        tiles = lax.fori_loop(first, last, listed, jnp.zeros((40, 64), f32))
        cells = jnp.dot(tiles.astype(jnp.bfloat16), widen, preferred_element_type=f32)
        for c in range(CH):
            table[c] = cells[:, c * LANES : (c + 1) * LANES]

    def layer_of(p):
        return jnp.where(core == 1, p, PZ - 1 - p)

    def flat(ref):
        return ref.reshape(CH, PZ * PX, LANES)

    ls_f, dv_f, air_f, dist_f, gain_f, q1_f, q2_f, z0_f, y_f = map(
        flat, (ls, dv, air, dist, gain, q1, q2, z0_ref, y_ref)
    )
    lane = lax.broadcasted_iota(jnp.int32, (8, LANES), 1)

    def rows_at(ref, r):
        return [ref[c, pl.ds(r, 8), :] for c in range(CH)]

    def beside(ref, r, middle):
        up = [pltpu.roll(v, LANES - 1, 1) for v in middle]
        down = [pltpu.roll(v, 1, 1) for v in middle]
        pieces = []
        for c in range(CH):
            after = up[c + 1] if c + 1 < CH else 0.0
            before = down[c - 1] if c > 0 else 0.0
            pieces.append(
                [
                    ref[c, pl.ds(r + 1, 8), :],
                    ref[c, pl.ds(r - 1, 8), :],
                    ref[c, pl.ds(r + PX, 8), :],
                    ref[c, pl.ds(r - PX, 8), :],
                    jnp.where(lane == LANES - 1, after, up[c]),
                    jnp.where(lane == 0, before, down[c]),
                ]
            )
        return pieces

    def added(parts):
        a, b, c, d, e, f = parts
        return ((a + b) + (c + d)) + (e + f)

    def walk(first, last, layer, held=0, group=3):
        rounds = (last - first + 1) // group

        def some(q, held):
            for step in range(group):
                held = layer(layer_of(first + q * group + step), held)
            return held

        if rounds > 1:
            held = lax.fori_loop(0, rounds, some, held)
            first = first + rounds * group
        for p in range(first, last + 1):
            held = layer(layer_of(p), held)
        return held

    def find_air(columns):
        def layer(z, carry):
            base = z * PX
            row_of = 10 * (
                (z >= Z0).astype(jnp.int32)
                + (z >= Z0 + 8).astype(jnp.int32)
                + (z >= Z0 + 16).astype(jnp.int32)
            )
            for j in columns:
                for c in range(CH):
                    level = ls_f[c, pl.ds(base + 8 * j, 8), :]
                    on = table[c, pl.ds(row_of + j, 1), :] > 0.5
                    fluid = jnp.logical_and(level < 0, on)
                    air_f[c, pl.ds(base + 8 * j, 8), :] = jnp.where(fluid, 0.0, jnp.abs(level))
                    dist_f[c, pl.ds(base + 8 * j, 8), :] = jnp.where(fluid, -level, 0.0)
            return carry

        return layer

    def find_gain(columns, with_q1=True):
        def layer(z, carry):
            base = z * PX + 4
            for i in columns:
                r = base + 8 * i
                middle = rows_at(air_f, r)
                for c, parts in enumerate(beside(air_f, r, middle)):
                    distance = dist_f[c, pl.ds(r, 8), :]
                    most = 19.0 * distance
                    extra = added([jnp.minimum(part, most) for part in parts])
                    below = jnp.maximum(6.0 * distance + extra, 0.1)
                    here = (2.0 / 3.0) * distance / below
                    gain_f[c, pl.ds(r, 8), :] = here
                    if with_q1:
                        q1_f[c, pl.ds(r, 8), :] = here * dv_f[c, pl.ds(r, 8), :]
            return carry

        return layer

    def find_q1(z, carry):
        for i in (0, WALK - 1):
            r = z * PX + 4 + 8 * i
            for c in range(CH):
                q1_f[c, pl.ds(r, 8), :] = gain_f[c, pl.ds(r, 8), :] * dv_f[c, pl.ds(r, 8), :]
        return carry

    def stage(source, target, own_part, sign, columns=range(WALK)):
        def layer(z, carry):
            base = z * PX + 4
            for i in columns:
                r = base + 8 * i
                middle = rows_at(source, r)
                for c, parts in enumerate(beside(source, r, middle)):
                    here = gain_f[c, pl.ds(r, 8), :] * added(parts)
                    target[c, pl.ds(r, 8), :] = own_part * middle[c] + sign * here
            return carry

        return layer

    def find_z0(columns=range(WALK)):
        return stage(q1_f, z0_f, 4.0 / 3.0, 1.0, columns)

    def find_q2(columns=range(WALK)):
        return stage(z0_f, q2_f, 2.0 / 3.0, -1.0, columns)

    find_y = stage(q2_f, y_f, 4.0 / 3.0, 1.0)

    def finish(z, held):
        base = z * PX + X0
        out = (z - Z0) * NX
        held = list(held)
        for i in range(NX // 8):
            r = base + 8 * i
            middle = rows_at(y_f, r)
            for c, parts in enumerate(beside(y_f, r, middle)):
                here = gain_f[c, pl.ds(r, 8), :]
                inverse = 1.0 / jnp.maximum(here, 1e-3)
                r0 = jnp.where(here > 0.0, dv_f[c, pl.ds(r, 8), :], 0.0)
                w0 = inverse * q2_f[c, pl.ds(r, 8), :]
                u = inverse * ((2.0 / 3.0) * middle[c] - here * added(parts))
                z0 = z0_f[c, pl.ds(r, 8), :]
                y = middle[c]
                r0_ref[c, pl.ds(out + 8 * i, 8), :] = r0
                w0_ref[c, pl.ds(out + 8 * i, 8), :] = w0
                u_ref[c, pl.ds(out + 8 * i, 8), :] = u
                r_s, z_s, w_s = r0 - SHIFT * w0, z0 - SHIFT * y, w0 - SHIFT * u
                products = (r0 * z0, w0 * z0, w0 * y, u * y, r_s * z_s, w_s * z_s)
                held = [total + term for total, term in zip(held, products)]
        return tuple(held)

    from_above = lambda sz: sz == -1
    from_below = lambda sz: sz == 1

    def arrive_at(side_of_even, side_of_odd, chosen):
        for parity, side in ((0, side_of_even), (1, side_of_odd)):

            @pl.when(core == parity)
            def _(side=side):
                arrive(lambda field, sx, sz, kx, kz, wave: side(sz) and chosen(field, sx, wave))

    def arrive_early(chosen):
        arrive_at(from_above, from_below, chosen)

    def arrive_late(chosen):
        arrive_at(from_below, from_above, chosen)

    every_column, inner = range(10), range(1, 9)
    edges, between = (0, WALK - 1), range(1, WALK - 1)
    fill_table(4, 5)
    walk(5, 20, find_air(inner))
    loaded(dv, 1, (0, 1))
    send(lambda field, sx, sz, kx, kz, wave: field == "dv" and sx == 0 and wave == 1)
    loaded(dv, 1, (2,))
    send(lambda field, sx, sz, kx, kz, wave: field == "dv" and sx != 0 and sz == 0)
    send(lambda field, sx, sz, kx, kz, wave: field == "dv" and sx != 0 and sz != 0)
    send(lambda field, sx, sz, kx, kz, wave: wave == 2)
    heed(0)
    walk(6, 19, find_gain(between))
    heed(1)
    for sx, sz in around:
        pl.when(exists(-sx, -sz))(lambda sx=sx, sz=sz: id_copy(sx, sz, -1).wait_recv())
    fill_table(0, 9)
    arrive_early(lambda field, sx, wave: sx == 0)
    walk(0, 4, find_air(inner))
    walk(1, 5, find_gain(between))
    heed(2)
    arrive(lambda field, sx, sz, kx, kz, wave: sz == 0 and field == "ls")
    arrive_early(lambda field, sx, wave: sx != 0 and field == "ls")
    walk(0, 20, find_air((0, 9)))
    walk(1, 19, find_gain(edges, False))
    heed(3)
    walk(2, 18, find_z0(range(2, 7)))
    walk(3, 17, find_q2(range(3, 6)), group=5)
    arrive(lambda field, sx, sz, kx, kz, wave: sz == 0 and field == "dv")
    arrive_early(lambda field, sx, wave: sx != 0 and field == "dv")
    heed(4)
    walk(1, 19, find_q1)
    walk(2, 18, find_z0((0, 1, 7, 8)), group=4)
    walk(3, 17, find_q2((0, 1, 2, 6, 7, 8)))
    heed(5)
    walk(4, 16, find_y)
    held = walk(5, 15, finish, tuple(jnp.zeros((8, LANES), f32) for _ in range(6)))

    heed(6)
    arrive_late(lambda field, sx, wave: wave == 1)
    walk(21, 24, find_air(every_column), group=2)
    walk(20, 23, find_gain(range(WALK)), group=2)
    walk(19, 22, find_z0(), group=2)
    walk(18, 21, find_q2(), group=2)
    walk(17, 20, find_y, group=2)
    held = walk(16, 19, finish, held, group=2)

    arrive_late(lambda field, sx, wave: wave == 2)
    walk(25, 25, find_air(every_column))
    walk(24, 24, find_gain(range(WALK)))
    walk(23, 23, find_z0())
    walk(22, 22, find_q2())
    walk(21, 21, find_y)
    held = walk(20, 20, finish, held)

    lane_row = lax.broadcasted_iota(jnp.int32, (1, LANES), 1)
    packed = jnp.zeros((1, LANES), f32)
    for k, total in enumerate(held):
        whole = jnp.sum(jnp.sum(total, axis=0, keepdims=True), axis=1, keepdims=True)
        packed = jnp.where(lane_row == k, whole, packed)

    def ring_distance(i):
        return sum((0, 1, 2, 1)[(i >> shift) & 3] for shift in (1, 3, 5))

    every_sum[pl.ds(0, 1), :] = packed
    for i in sorted(range(1, DEVICES), key=lambda i: -ring_distance(i)):
        pltpu.make_async_remote_copy(
            every_sum.at[pl.ds(0, 1)], every_sum.at[pl.ds(i, 1)], ar_send.at[0], ar_recv.at[0],
            device_id=sum_peer(i), device_id_type=MESH,
        ).start()
    sent = pltpu.make_async_remote_copy(
        every_sum.at[pl.ds(0, DEVICES - 1)], every_sum.at[pl.ds(1, DEVICES - 1)], ar_send.at[0], ar_recv.at[0],
        device_id=sum_peer(1), device_id_type=MESH,
    )
    sent.wait_recv()
    sums[pl.ds(0, 1), :] = jnp.sum(every_sum[...], axis=0, keepdims=True)
    gamma0, delta0, eta, theta, gamma_s, delta_s = (sums[pl.ds(0, 1), pl.ds(k, 1)] for k in range(6))
    alpha0 = gamma0 / delta0
    off = alpha0 - SHIFT
    kappa, lam = delta0 - SHIFT * eta, eta - SHIFT * theta
    gamma1 = gamma_s - 2.0 * off * kappa + off * off * eta
    delta1 = delta_s - 2.0 * off * lam + off * off * theta
    beta = gamma1 / gamma0
    below = delta1 - beta * gamma1 / alpha0
    alpha1 = jnp.where(below > 0, gamma1 / jnp.where(below > 0, below, 1.0), 0.0)
    for k, value in enumerate((alpha0, alpha1, beta)):
        step_ref[k] = jnp.broadcast_to(value, (8, LANES))

    for number, message in enumerate(MESSAGES):
        _, sx, sz, _, _, _ = message
        pl.when(exists(sx, sz))(lambda number=number: layer_copy(number).wait_send())
    for sx, sz in around:
        pl.when(exists(sx, sz))(lambda sx=sx, sz=sz: id_copy(sx, sz).wait_send())
    sent.wait_send()


def last_kernel(z0_ref, y_ref, r0_ref, w0_ref, u_ref, step_ref, p_out, r_out, p_buf, r_buf, sem):
    alpha0, alpha1, beta = step_ref[0], step_ref[1], step_ref[2]
    z0_f = z0_ref.reshape(CH, PZ * PX, LANES)
    y_f = y_ref.reshape(CH, PZ * PX, LANES)
    p_f = p_buf.reshape(CH, NZ * NX, LANES)
    r_f = r_buf.reshape(CH, NZ * NX, LANES)

    for z in range(NZ):
        def rows(i, carry, z=z):
            wide = (Z0 + z) * PX + X0 + 8 * i
            r = z * NX + 8 * i
            for c in range(CH):
                z0 = z0_f[c, pl.ds(wide, 8), :]
                z1 = z0 - alpha0 * y_f[c, pl.ds(wide, 8), :]
                p_f[c, pl.ds(r, 8), :] = alpha0 * z0 + alpha1 * (z1 + beta * z0)
                w0 = w0_ref[c, pl.ds(r, 8), :]
                w1 = w0 - alpha0 * u_ref[c, pl.ds(r, 8), :]
                r1 = r0_ref[c, pl.ds(r, 8), :] - alpha0 * w0
                r_f[c, pl.ds(r, 8), :] = r1 - alpha1 * (w1 + beta * w0)
            return carry

        lax.fori_loop(0, NX // 8, rows, 0, unroll=True)
        for number, (buffer, target) in enumerate(((p_buf, p_out), (r_buf, r_out))):
            for c in range(CH):
                pltpu.make_async_copy(
                    buffer.at[c, z], target.at[:, z, pl.ds(c * LANES, LANES)], sem.at[number]
                ).start()
    for number, buffer in enumerate((p_buf, r_buf)):
        pltpu.make_async_copy(buffer, buffer, sem.at[number]).wait()


def on_device(divergence, level_set, tile_ids):
    extended = (CH, PZ, PX, LANES)
    block = (CH, NZ * NX, LANES)
    held = pl.pallas_call(
        main_kernel,
        out_shape=[pltpu.VMEM(extended, f32)] * 2 + [pltpu.VMEM(block, f32)] * 3 + [pltpu.VMEM((3, 8, LANES), f32)],
        in_specs=[pl.BlockSpec(memory_space=pltpu.HBM)] * 3,
        out_specs=[pl.BlockSpec(memory_space=pltpu.VMEM)] * 6,
        scratch_shapes=[
            *[pltpu.VMEM(extended, f32)] * 7,
            pltpu.VMEM((9, 1, SLOTS), jnp.int32),
            pltpu.VMEM((CH, 40, LANES), f32),
            pltpu.VMEM((8, LANES), f32),
            pltpu.VMEM((DEVICES, LANES), f32),
            pltpu.SemaphoreType.DMA((7,)),
            pltpu.SemaphoreType.DMA((len(MESSAGES),)),
            pltpu.SemaphoreType.DMA((len(MESSAGES),)),
            pltpu.SemaphoreType.DMA((9,)),
            pltpu.SemaphoreType.DMA((9,)),
            pltpu.SemaphoreType.DMA((1,)),
            pltpu.SemaphoreType.DMA((1,)),
            pltpu.SemaphoreType.REGULAR((7,)),
        ],
        compiler_params=pltpu.CompilerParams(
            collective_id=0, has_side_effects=True, vmem_limit_bytes=40 * 2**20
        ),
        name="solve",
    )(*(pltpu.with_memory_space_constraint(array, pltpu.HBM) for array in (divergence, level_set, tile_ids)))
    return pl.pallas_call(
        last_kernel,
        out_shape=[jax.ShapeDtypeStruct(divergence.shape, f32)] * 2,
        in_specs=[pl.BlockSpec(memory_space=pltpu.VMEM)] * 6,
        out_specs=[pl.BlockSpec(memory_space=pl.ANY)] * 2,
        scratch_shapes=[
            pltpu.VMEM((CH, NZ, NX, LANES), f32),
            pltpu.VMEM((CH, NZ, NX, LANES), f32),
            pltpu.SemaphoreType.DMA((2,)),
        ],
        compiler_params=pltpu.CompilerParams(vmem_limit_bytes=12 * 2**20),
        name="update",
    )(*held)


def solution(mesh):
    return jax.shard_map(
        on_device,
        mesh=mesh,
        in_specs=(P("gx", "gz", None), P("gx", "gz", None), P("gx", "gz")),
        out_specs=(P("gx", "gz", None), P("gx", "gz", None)),
        check_vma=False,
    )
```

```python
import functools

import jax
import jax.numpy as jnp
from jax import lax
from jax.experimental import pallas as pl
from jax.experimental.pallas import tpu as pltpu
from jax.sharding import PartitionSpec as P

MESH = pl.DeviceIdType.MESH
f32 = jnp.float32

CH, LANES = 4, 128
NX, NZ = 64, 16
X0, Z0 = 8, 5
PX, PZ = 80, 26
N_GX, N_GZ = 4, 32
DEVICES = N_GX * N_GZ
SLOTS = 1024
SHIFT = 1.125
WALK = 9


def span(axis_len, origin, sign, near, far):
    if sign == 0:
        return origin, origin, axis_len
    if sign > 0:
        return origin + axis_len - far, origin - far, far - near + 1
    return origin - 1 + near, origin + axis_len - 1 + near, far - near + 1


def message_list():
    every = []
    for sx in (-1, 1):
        every.append(("ls", sx, 0, (1, 5), None, 0))
        every.append(("dv", sx, 0, (1, 4), None, 0))
    for sz in (-1, 1):
        every.append(("ls", 0, sz, None, (1, 4), 1))
        every.append(("dv", 0, sz, None, (1, 3), 1))
        every.append(("ls", 0, sz, None, (5, 5), 2))
        every.append(("dv", 0, sz, None, (4, 4), 2))
        for sx in (-1, 1):
            every.append(("ls", sx, sz, (1, 4), (1, 2), 1))
            every.append(("ls", sx, sz, (1, 2), (3, 4), 1))
            every.append(("dv", sx, sz, (1, 3), (1, 1), 1))
            every.append(("dv", sx, sz, (1, 2), (2, 3), 1))
    return every


MESSAGES = message_list()
AROUND = [(sx, sz) for sx in (-1, 0, 1) for sz in (-1, 0, 1)]


def main_kernel(
    dv_in, ls_in, ids_in,
    z0_ref, y_ref, r0_ref, w0_ref, u_ref, step_ref,
    ls, dv, air, dist, gain, q1, q2, ids, table, sums, every_sum,
    load_sem, send_sem, recv_sem, id_send, id_recv, ar_send, ar_recv, word_sem,
):
    gx, gz = lax.axis_index("gx"), lax.axis_index("gz")
    core = lax.rem(gz, 2)
    place_z = lax.rem(gz // 2, 4)
    place_x = gz // 8

    def exists(sx, sz):
        ok = None
        for position, count, sign in ((gx, N_GX, sx), (gz, N_GZ, sz)):
            if sign:
                here = position < count - 1 if sign > 0 else position > 0
                ok = here if ok is None else jnp.logical_and(ok, here)
        return ok

    for k in range(9):
        if k != 4:
            ids[k] = jnp.full((1, SLOTS), -1, jnp.int32)

    def clear(z_first, z_count, x_first, x_count):
        def layer(z, carry):
            for array in (ls, dv):
                for c in range(CH):
                    array[c, z, pl.ds(x_first, x_count), :] = jnp.zeros((x_count, LANES), f32)
            return carry

        lax.fori_loop(z_first, z_first + z_count, layer, 0)

    pl.when(gx == 0)(lambda: clear(0, PZ, 0, X0))
    pl.when(gx == N_GX - 1)(lambda: clear(0, PZ, X0 + NX, 8))
    pl.when(gz == 0)(lambda: clear(0, Z0, 0, PX))
    pl.when(gz == N_GZ - 1)(lambda: clear(Z0 + NZ, 5, 0, PX))

    me_chip = (gx * 4 + place_x) * 4 + place_z

    def sum_peer(i):
        chip = me_chip ^ (i >> 1)
        return chip // 16, lax.rem(chip, 16) * 2 + (core ^ (i & 1))

    barrier = pltpu.get_barrier_semaphore()
    around = [(sx, sz) for sx, sz in AROUND if (sx, sz) != (0, 0)]
    for sx, sz in around:
        pl.when(exists(sx, sz))(
            lambda sx=sx, sz=sz: pl.semaphore_signal(
                barrier, inc=1, device_id=(gx + sx, gz + sz), device_id_type=MESH
            )
        )
    own_ids = pltpu.make_async_copy(ids_in, ids.at[4], load_sem.at[6])
    own_ids.start()
    parts = ((0, 5), (11, 5), (5, 6))
    for field, (source, target) in enumerate(((ls_in, ls), (dv_in, dv))):
        for part, (first, count) in enumerate(parts):
            for z in range(first, first + count):
                for c in range(CH):
                    pltpu.make_async_copy(
                        source.at[:, z, pl.ds(c * LANES, LANES)],
                        target.at[c, Z0 + z, pl.ds(X0, NX)],
                        load_sem.at[field * 3 + part],
                    ).start()

    def loaded(array, field, chosen):
        for part in chosen:
            first, count = parts[part]
            region = array.at[:, pl.ds(Z0 + first, count), pl.ds(X0, NX)]
            pltpu.make_async_copy(region, region, load_sem.at[field * 3 + part]).wait()

    peers = 0
    for sx, sz in around:
        peers = peers + exists(sx, sz).astype(jnp.int32)
    pl.semaphore_wait(barrier, peers)

    reach = [(0, 1), (0, 2), (0, 4), (0, 8), (0, 16), (1, 0), (2, 0)]

    def greeted(step):
        dx, dz = reach[step]
        for sign in (-1, 1):
            if dx:
                ok = gx + dx < N_GX if sign > 0 else gx >= dx
            else:
                ok = gz + dz < N_GZ if sign > 0 else gz >= dz
            yield ok, (gx + sign * dx, gz + sign * dz)

    def greet(step):
        for ok, peer in greeted(step):
            pl.when(ok)(
                lambda peer=peer: pl.semaphore_signal(
                    word_sem.at[step], inc=1, device_id=peer, device_id_type=MESH
                )
            )

    def heed(step):
        count = 0
        for ok, _ in greeted(step):
            count = count + ok.astype(jnp.int32)
        pl.semaphore_wait(word_sem.at[step], count)
        if step + 1 < len(reach):
            greet(step + 1)

    greet(0)

    def id_copy(sx, sz, peer=1):
        target = (1 - sx) * 3 + (1 - sz)
        return pltpu.make_async_remote_copy(
            ids.at[4], ids.at[target], id_send.at[target], id_recv.at[target],
            device_id=(gx + peer * sx, gz + peer * sz), device_id_type=MESH,
        )

    def layer_copy(number, peer=1):
        field, sx, sz, kx, kz, _ = MESSAGES[number]
        array = ls if field == "ls" else dv
        x_from, x_to, x_len = span(NX, X0, sx, *(kx or (0, 0)))
        z_from, z_to, z_len = span(NZ, Z0, sz, *(kz or (0, 0)))
        return pltpu.make_async_remote_copy(
            array.at[:, pl.ds(z_from, z_len), pl.ds(x_from, x_len)],
            array.at[:, pl.ds(z_to, z_len), pl.ds(x_to, x_len)],
            send_sem.at[number], recv_sem.at[number],
            device_id=(gx + peer * sx, gz + peer * sz), device_id_type=MESH,
        )

    def send(chosen):
        for number, message in enumerate(MESSAGES):
            if chosen(*message):
                _, sx, sz, _, _, _ = message
                pl.when(exists(sx, sz))(lambda number=number: layer_copy(number).start())

    def arrive(chosen):
        for number, message in enumerate(MESSAGES):
            if chosen(*message):
                _, sx, sz, _, _, _ = message
                pl.when(exists(-sx, -sz))(lambda number=number: layer_copy(number, -1).wait_recv())

    own_ids.wait()
    for sx, sz in around:
        pl.when(exists(sx, sz))(lambda sx=sx, sz=sz: id_copy(sx, sz).start())
    loaded(ls, 0, (0, 1))
    send(lambda field, sx, sz, kx, kz, wave: field == "ls" and sx == 0 and wave == 1)
    loaded(ls, 0, (2,))
    send(lambda field, sx, sz, kx, kz, wave: field == "ls" and sx != 0 and sz == 0)
    send(lambda field, sx, sz, kx, kz, wave: field == "ls" and sx != 0 and sz != 0)

    row = lax.broadcasted_iota(jnp.int32, (40, 1), 0)
    row_z = (row >= 10).astype(jnp.int32) + (row >= 20).astype(jnp.int32) + (row >= 30).astype(jnp.int32)
    row_x = row - 10 * row_z
    from_device = (
        jnp.where(row_x == 0, 0, jnp.where(row_x == 9, 2, 1)) * 3
        + jnp.where(row_z == 0, 0, jnp.where(row_z == 3, 2, 1))
    )
    tile_x = jnp.where(row_x == 0, 7, jnp.where(row_x == 9, 0, row_x - 1))
    tile_z = jnp.where(row_z == 0, 1, jnp.where(row_z == 3, 0, row_z - 1))
    code = tile_x * 2 + tile_z

    def listed(k, total):
        numbers = ids[k]
        wanted = jnp.where(from_device == k, code, -2)
        rows_hit = jnp.where((numbers >> 6) == wanted, 1.0, 0.0).astype(jnp.bfloat16)
        tile_y = lax.broadcasted_iota(jnp.int32, (64, 1), 0)
        y_hit = jnp.where((numbers & 63) == tile_y, 1.0, 0.0).astype(jnp.bfloat16)
        return total + lax.dot_general(
            rows_hit, y_hit, (((1,), (1,)), ((), ())), preferred_element_type=f32
        )

    widen = lax.broadcasted_iota(jnp.int32, (64, CH * LANES), 1) >> 3
    widen = jnp.where(widen == lax.broadcasted_iota(jnp.int32, (64, CH * LANES), 0), 1.0, 0.0)
    widen = widen.astype(jnp.bfloat16)

    def fill_table(first, last):
        tiles = lax.fori_loop(first, last, listed, jnp.zeros((40, 64), f32))
        cells = jnp.dot(tiles.astype(jnp.bfloat16), widen, preferred_element_type=f32)
        for c in range(CH):
            table[c] = cells[:, c * LANES : (c + 1) * LANES]

    def layer_of(p):
        return jnp.where(core == 1, p, PZ - 1 - p)

    def flat(ref):
        return ref.reshape(CH, PZ * PX, LANES)

    ls_f, dv_f, air_f, dist_f, gain_f, q1_f, q2_f, z0_f, y_f = map(
        flat, (ls, dv, air, dist, gain, q1, q2, z0_ref, y_ref)
    )
    lane = lax.broadcasted_iota(jnp.int32, (8, LANES), 1)

    def rows_at(ref, r):
        return [ref[c, pl.ds(r, 8), :] for c in range(CH)]

    def beside(ref, r, middle):
        up = [pltpu.roll(v, LANES - 1, 1) for v in middle]
        down = [pltpu.roll(v, 1, 1) for v in middle]
        pieces = []
        for c in range(CH):
            after = up[c + 1] if c + 1 < CH else 0.0
            before = down[c - 1] if c > 0 else 0.0
            pieces.append(
                [
                    ref[c, pl.ds(r + 1, 8), :],
                    ref[c, pl.ds(r - 1, 8), :],
                    ref[c, pl.ds(r + PX, 8), :],
                    ref[c, pl.ds(r - PX, 8), :],
                    jnp.where(lane == LANES - 1, after, up[c]),
                    jnp.where(lane == 0, before, down[c]),
                ]
            )
        return pieces

    def added(parts):
        a, b, c, d, e, f = parts
        return ((a + b) + (c + d)) + (e + f)

    def walk(first, last, layer, held=0, group=3):
        rounds = (last - first + 1) // group

        def some(q, held):
            for step in range(group):
                held = layer(layer_of(first + q * group + step), held)
            return held

        if rounds > 1:
            held = lax.fori_loop(0, rounds, some, held)
            first = first + rounds * group
        for p in range(first, last + 1):
            held = layer(layer_of(p), held)
        return held

    def find_air(columns):
        def layer(z, carry):
            base = z * PX
            row_of = 10 * (
                (z >= Z0).astype(jnp.int32)
                + (z >= Z0 + 8).astype(jnp.int32)
                + (z >= Z0 + 16).astype(jnp.int32)
            )
            for j in columns:
                for c in range(CH):
                    level = ls_f[c, pl.ds(base + 8 * j, 8), :]
                    on = table[c, pl.ds(row_of + j, 1), :] > 0.5
                    fluid = jnp.logical_and(level < 0, on)
                    air_f[c, pl.ds(base + 8 * j, 8), :] = jnp.where(fluid, 0.0, jnp.abs(level))
                    dist_f[c, pl.ds(base + 8 * j, 8), :] = jnp.where(fluid, -level, 0.0)
            return carry

        return layer

    def find_gain(columns, with_q1=True):
        def layer(z, carry):
            base = z * PX + 4
            for i in columns:
                r = base + 8 * i
                middle = rows_at(air_f, r)
                for c, parts in enumerate(beside(air_f, r, middle)):
                    distance = dist_f[c, pl.ds(r, 8), :]
                    most = 19.0 * distance
                    extra = added([jnp.minimum(part, most) for part in parts])
                    below = jnp.maximum(6.0 * distance + extra, 0.1)
                    here = (2.0 / 3.0) * distance / below
                    gain_f[c, pl.ds(r, 8), :] = here
                    if with_q1:
                        q1_f[c, pl.ds(r, 8), :] = here * dv_f[c, pl.ds(r, 8), :]
            return carry

        return layer

    def find_q1(z, carry):
        for i in (0, WALK - 1):
            r = z * PX + 4 + 8 * i
            for c in range(CH):
                q1_f[c, pl.ds(r, 8), :] = gain_f[c, pl.ds(r, 8), :] * dv_f[c, pl.ds(r, 8), :]
        return carry

    def stage(source, target, own_part, sign, columns=range(WALK)):
        def layer(z, carry):
            base = z * PX + 4
            for i in columns:
                r = base + 8 * i
                middle = rows_at(source, r)
                for c, parts in enumerate(beside(source, r, middle)):
                    here = gain_f[c, pl.ds(r, 8), :] * added(parts)
                    target[c, pl.ds(r, 8), :] = own_part * middle[c] + sign * here
            return carry

        return layer

    def find_z0(columns=range(WALK)):
        return stage(q1_f, z0_f, 4.0 / 3.0, 1.0, columns)

    def find_q2(columns=range(WALK)):
        return stage(z0_f, q2_f, 2.0 / 3.0, -1.0, columns)

    find_y = stage(q2_f, y_f, 4.0 / 3.0, 1.0)

    def finish(z, held):
        base = z * PX + X0
        out = (z - Z0) * NX
        held = list(held)
        for i in range(NX // 8):
            r = base + 8 * i
            middle = rows_at(y_f, r)
            for c, parts in enumerate(beside(y_f, r, middle)):
                here = gain_f[c, pl.ds(r, 8), :]
                inverse = 1.0 / jnp.maximum(here, 1e-3)
                r0 = jnp.where(here > 0.0, dv_f[c, pl.ds(r, 8), :], 0.0)
                w0 = inverse * q2_f[c, pl.ds(r, 8), :]
                u = inverse * ((2.0 / 3.0) * middle[c] - here * added(parts))
                z0 = z0_f[c, pl.ds(r, 8), :]
                y = middle[c]
                r0_ref[c, pl.ds(out + 8 * i, 8), :] = r0
                w0_ref[c, pl.ds(out + 8 * i, 8), :] = w0
                u_ref[c, pl.ds(out + 8 * i, 8), :] = u
                z_s = z0 - SHIFT * y
                products = (r0 * z0, w0 * z0, r0 * z_s, w0 * z_s, u * z_s)
                held = [total + term for total, term in zip(held, products)]
        return tuple(held)

    from_above = lambda sz: sz == -1
    from_below = lambda sz: sz == 1

    def arrive_at(side_of_even, side_of_odd, chosen):
        for parity, side in ((0, side_of_even), (1, side_of_odd)):

            @pl.when(core == parity)
            def _(side=side):
                arrive(lambda field, sx, sz, kx, kz, wave: side(sz) and chosen(field, sx, wave))

    def arrive_early(chosen):
        arrive_at(from_above, from_below, chosen)

    def arrive_late(chosen):
        arrive_at(from_below, from_above, chosen)

    every_column, inner = range(10), range(1, 9)
    edges, between = (0, WALK - 1), range(1, WALK - 1)
    fill_table(4, 5)
    walk(5, 20, find_air(inner))
    loaded(dv, 1, (0, 1))
    send(lambda field, sx, sz, kx, kz, wave: field == "dv" and sx == 0 and wave == 1)
    loaded(dv, 1, (2,))
    send(lambda field, sx, sz, kx, kz, wave: field == "dv" and sx != 0 and sz == 0)
    send(lambda field, sx, sz, kx, kz, wave: field == "dv" and sx != 0 and sz != 0)
    send(lambda field, sx, sz, kx, kz, wave: wave == 2)
    heed(0)
    walk(6, 19, find_gain(between))
    heed(1)
    for sx, sz in around:
        pl.when(exists(-sx, -sz))(lambda sx=sx, sz=sz: id_copy(sx, sz, -1).wait_recv())
    fill_table(0, 9)
    arrive_early(lambda field, sx, wave: sx == 0)
    walk(0, 4, find_air(inner))
    walk(1, 5, find_gain(between))
    heed(2)
    arrive(lambda field, sx, sz, kx, kz, wave: sz == 0 and field == "ls")
    arrive_early(lambda field, sx, wave: sx != 0 and field == "ls")
    walk(0, 20, find_air((0, 9)))
    walk(1, 19, find_gain(edges, False))
    heed(3)
    walk(2, 18, find_z0(range(2, 7)), group=6)
    walk(3, 17, find_q2(range(3, 6)), group=5)
    arrive(lambda field, sx, sz, kx, kz, wave: sz == 0 and field == "dv")
    arrive_early(lambda field, sx, wave: sx != 0 and field == "dv")
    heed(4)
    walk(1, 19, find_q1)
    walk(2, 18, find_z0((0, 1, 7, 8)), group=6)
    walk(3, 17, find_q2((0, 1, 2, 6, 7, 8)), group=5)
    heed(5)
    walk(4, 16, find_y, group=5)
    held = walk(5, 15, finish, tuple(jnp.zeros((8, LANES), f32) for _ in range(5)), group=3)

    heed(6)
    arrive_late(lambda field, sx, wave: wave == 1)
    walk(21, 24, find_air(every_column), group=2)
    walk(20, 23, find_gain(range(WALK)), group=2)
    walk(19, 22, find_z0(), group=4)
    walk(18, 21, find_q2(), group=4)
    walk(17, 20, find_y, group=4)
    held = walk(16, 19, finish, held, group=2)

    arrive_late(lambda field, sx, wave: wave == 2)
    walk(25, 25, find_air(every_column))
    walk(24, 24, find_gain(range(WALK)))
    walk(23, 23, find_z0())
    walk(22, 22, find_q2())
    walk(21, 21, find_y)
    held = walk(20, 20, finish, held)

    lane_row = lax.broadcasted_iota(jnp.int32, (1, LANES), 1)
    packed = jnp.zeros((1, LANES), f32)
    for k, total in enumerate(held):
        whole = jnp.sum(jnp.sum(total, axis=0, keepdims=True), axis=1, keepdims=True)
        packed = jnp.where(lane_row == k, whole, packed)

    def ring_distance(i):
        return sum((0, 1, 2, 1)[(i >> shift) & 3] for shift in (1, 3, 5))

    every_sum[pl.ds(0, 1), :] = packed
    for i in sorted(range(1, DEVICES), key=lambda i: -ring_distance(i)):
        pltpu.make_async_remote_copy(
            every_sum.at[pl.ds(0, 1)], every_sum.at[pl.ds(i, 1)], ar_send.at[0], ar_recv.at[0],
            device_id=sum_peer(i), device_id_type=MESH,
        ).start()
    sent = pltpu.make_async_remote_copy(
        every_sum.at[pl.ds(0, DEVICES - 1)], every_sum.at[pl.ds(1, DEVICES - 1)], ar_send.at[0], ar_recv.at[0],
        device_id=sum_peer(1), device_id_type=MESH,
    )
    sent.wait_recv()
    sums[pl.ds(0, 1), :] = jnp.sum(every_sum[...], axis=0, keepdims=True)
    gamma0, delta0, first, kappa, lam = (sums[pl.ds(0, 1), pl.ds(k, 1)] for k in range(5))
    eta = (delta0 - kappa) / SHIFT
    theta = (eta - lam) / SHIFT
    gamma_s, delta_s = first - SHIFT * kappa, kappa - SHIFT * lam
    alpha0 = gamma0 / delta0
    off = alpha0 - SHIFT
    gamma1 = gamma_s - 2.0 * off * kappa + off * off * eta
    delta1 = delta_s - 2.0 * off * lam + off * off * theta
    beta = gamma1 / gamma0
    below = delta1 - beta * gamma1 / alpha0
    alpha1 = jnp.where(below > 0, gamma1 / jnp.where(below > 0, below, 1.0), 0.0)
    for k, value in enumerate((alpha0, alpha1, beta)):
        step_ref[k] = jnp.broadcast_to(value, (8, LANES))

    for number, message in enumerate(MESSAGES):
        _, sx, sz, _, _, _ = message
        pl.when(exists(sx, sz))(lambda number=number: layer_copy(number).wait_send())
    for sx, sz in around:
        pl.when(exists(sx, sz))(lambda sx=sx, sz=sz: id_copy(sx, sz).wait_send())
    sent.wait_send()


def last_kernel(z0_ref, y_ref, r0_ref, w0_ref, u_ref, step_ref, p_out, r_out, p_buf, r_buf, sem):
    alpha0, alpha1, beta = step_ref[0], step_ref[1], step_ref[2]
    z0_f = z0_ref.reshape(CH, PZ * PX, LANES)
    y_f = y_ref.reshape(CH, PZ * PX, LANES)
    p_f = p_buf.reshape(CH, NZ * NX, LANES)
    r_f = r_buf.reshape(CH, NZ * NX, LANES)

    for z in range(NZ):
        def rows(i, carry, z=z):
            wide = (Z0 + z) * PX + X0 + 8 * i
            r = z * NX + 8 * i
            for c in range(CH):
                z0 = z0_f[c, pl.ds(wide, 8), :]
                z1 = z0 - alpha0 * y_f[c, pl.ds(wide, 8), :]
                p_f[c, pl.ds(r, 8), :] = alpha0 * z0 + alpha1 * (z1 + beta * z0)
                w0 = w0_ref[c, pl.ds(r, 8), :]
                w1 = w0 - alpha0 * u_ref[c, pl.ds(r, 8), :]
                r1 = r0_ref[c, pl.ds(r, 8), :] - alpha0 * w0
                r_f[c, pl.ds(r, 8), :] = r1 - alpha1 * (w1 + beta * w0)
            return carry

        lax.fori_loop(0, NX // 8, rows, 0, unroll=True)
        for number, (buffer, target) in enumerate(((p_buf, p_out), (r_buf, r_out))):
            for c in range(CH):
                pltpu.make_async_copy(
                    buffer.at[c, z], target.at[:, z, pl.ds(c * LANES, LANES)], sem.at[number]
                ).start()
    for number, buffer in enumerate((p_buf, r_buf)):
        pltpu.make_async_copy(buffer, buffer, sem.at[number]).wait()


def on_device(divergence, level_set, tile_ids):
    extended = (CH, PZ, PX, LANES)
    block = (CH, NZ * NX, LANES)
    held = pl.pallas_call(
        main_kernel,
        out_shape=[pltpu.VMEM(extended, f32)] * 2 + [pltpu.VMEM(block, f32)] * 3 + [pltpu.VMEM((3, 8, LANES), f32)],
        in_specs=[pl.BlockSpec(memory_space=pltpu.HBM)] * 3,
        out_specs=[pl.BlockSpec(memory_space=pltpu.VMEM)] * 6,
        scratch_shapes=[
            *[pltpu.VMEM(extended, f32)] * 7,
            pltpu.VMEM((9, 1, SLOTS), jnp.int32),
            pltpu.VMEM((CH, 40, LANES), f32),
            pltpu.VMEM((8, LANES), f32),
            pltpu.VMEM((DEVICES, LANES), f32),
            pltpu.SemaphoreType.DMA((7,)),
            pltpu.SemaphoreType.DMA((len(MESSAGES),)),
            pltpu.SemaphoreType.DMA((len(MESSAGES),)),
            pltpu.SemaphoreType.DMA((9,)),
            pltpu.SemaphoreType.DMA((9,)),
            pltpu.SemaphoreType.DMA((1,)),
            pltpu.SemaphoreType.DMA((1,)),
            pltpu.SemaphoreType.REGULAR((7,)),
        ],
        compiler_params=pltpu.CompilerParams(
            collective_id=0, has_side_effects=True, vmem_limit_bytes=40 * 2**20
        ),
        name="solve",
    )(*(pltpu.with_memory_space_constraint(array, pltpu.HBM) for array in (divergence, level_set, tile_ids)))
    return pl.pallas_call(
        last_kernel,
        out_shape=[jax.ShapeDtypeStruct(divergence.shape, f32)] * 2,
        in_specs=[pl.BlockSpec(memory_space=pltpu.VMEM)] * 6,
        out_specs=[pl.BlockSpec(memory_space=pl.ANY)] * 2,
        scratch_shapes=[
            pltpu.VMEM((CH, NZ, NX, LANES), f32),
            pltpu.VMEM((CH, NZ, NX, LANES), f32),
            pltpu.SemaphoreType.DMA((2,)),
        ],
        compiler_params=pltpu.CompilerParams(vmem_limit_bytes=12 * 2**20),
        name="update",
    )(*held)


def solution(mesh):
    return jax.shard_map(
        on_device,
        mesh=mesh,
        in_specs=(P("gx", "gz", None), P("gx", "gz", None), P("gx", "gz")),
        out_specs=(P("gx", "gz", None), P("gx", "gz", None)),
        check_vma=False,
    )
```

```python
import functools

import jax
import jax.numpy as jnp
from jax import lax
from jax.experimental import pallas as pl
from jax.experimental.pallas import tpu as pltpu
from jax.sharding import PartitionSpec as P

MESH = pl.DeviceIdType.MESH
f32 = jnp.float32

CH, LANES = 4, 128
NX, NZ = 64, 16
X0, Z0 = 8, 5
PX, PZ = 80, 26
N_GX, N_GZ = 4, 32
DEVICES = N_GX * N_GZ
SLOTS = 1024
SHIFT = 1.125
WALK = 9


def span(axis_len, origin, sign, near, far):
    if sign == 0:
        return origin, origin, axis_len
    if sign > 0:
        return origin + axis_len - far, origin - far, far - near + 1
    return origin - 1 + near, origin + axis_len - 1 + near, far - near + 1


def message_list():
    every = []
    for sx in (-1, 1):
        every.append(("ls", sx, 0, (1, 5), None, 0))
        every.append(("dv", sx, 0, (1, 4), None, 0))
    for sz in (-1, 1):
        every.append(("ls", 0, sz, None, (1, 4), 1))
        every.append(("dv", 0, sz, None, (1, 3), 1))
        every.append(("ls", 0, sz, None, (5, 5), 2))
        every.append(("dv", 0, sz, None, (4, 4), 2))
        for sx in (-1, 1):
            every.append(("ls", sx, sz, (1, 4), (1, 2), 1))
            every.append(("ls", sx, sz, (1, 2), (3, 4), 1))
            every.append(("dv", sx, sz, (1, 3), (1, 1), 1))
            every.append(("dv", sx, sz, (1, 2), (2, 3), 1))
    return every


MESSAGES = message_list()
AROUND = [(sx, sz) for sx in (-1, 0, 1) for sz in (-1, 0, 1)]


def main_kernel(
    dv_in, ls_in, ids_in,
    z0_ref, y_ref, r0_ref, w0_ref, u_ref, step_ref,
    ls, dv, air, dist, gain, q1, q2, ids, table, sums, every_sum,
    load_sem, send_sem, recv_sem, id_send, id_recv, ar_send, ar_recv, word_sem,
):
    gx, gz = lax.axis_index("gx"), lax.axis_index("gz")
    core = lax.rem(gz, 2)
    place_z = lax.rem(gz // 2, 4)
    place_x = gz // 8

    def exists(sx, sz):
        ok = None
        for position, count, sign in ((gx, N_GX, sx), (gz, N_GZ, sz)):
            if sign:
                here = position < count - 1 if sign > 0 else position > 0
                ok = here if ok is None else jnp.logical_and(ok, here)
        return ok

    for k in range(9):
        if k != 4:
            ids[k] = jnp.full((1, SLOTS), -1, jnp.int32)

    def clear(z_first, z_count, x_first, x_count):
        def layer(z, carry):
            for array in (ls, dv):
                for c in range(CH):
                    array[c, z, pl.ds(x_first, x_count), :] = jnp.zeros((x_count, LANES), f32)
            return carry

        lax.fori_loop(z_first, z_first + z_count, layer, 0)

    pl.when(gx == 0)(lambda: clear(0, PZ, 0, X0))
    pl.when(gx == N_GX - 1)(lambda: clear(0, PZ, X0 + NX, 8))
    pl.when(gz == 0)(lambda: clear(0, Z0, 0, PX))
    pl.when(gz == N_GZ - 1)(lambda: clear(Z0 + NZ, 5, 0, PX))

    me_chip = (gx * 4 + place_x) * 4 + place_z

    def sum_peer(i):
        chip = me_chip ^ (i >> 1)
        return chip // 16, lax.rem(chip, 16) * 2 + (core ^ (i & 1))

    barrier = pltpu.get_barrier_semaphore()
    around = [(sx, sz) for sx, sz in AROUND if (sx, sz) != (0, 0)]
    for sx, sz in around:
        pl.when(exists(sx, sz))(
            lambda sx=sx, sz=sz: pl.semaphore_signal(
                barrier, inc=1, device_id=(gx + sx, gz + sz), device_id_type=MESH
            )
        )
    own_ids = pltpu.make_async_copy(ids_in, ids.at[4], load_sem.at[6])
    own_ids.start()
    parts = ((0, 5), (11, 5), (5, 6))
    for field, (source, target) in enumerate(((ls_in, ls), (dv_in, dv))):
        for part, (first, count) in enumerate(parts):
            for z in range(first, first + count):
                for c in range(CH):
                    pltpu.make_async_copy(
                        source.at[:, z, pl.ds(c * LANES, LANES)],
                        target.at[c, Z0 + z, pl.ds(X0, NX)],
                        load_sem.at[field * 3 + part],
                    ).start()

    def loaded(array, field, chosen):
        for part in chosen:
            first, count = parts[part]
            region = array.at[:, pl.ds(Z0 + first, count), pl.ds(X0, NX)]
            pltpu.make_async_copy(region, region, load_sem.at[field * 3 + part]).wait()

    peers = 0
    for sx, sz in around:
        peers = peers + exists(sx, sz).astype(jnp.int32)
    pl.semaphore_wait(barrier, peers)

    reach = [(0, 1), (0, 2), (0, 4), (0, 8), (0, 16), (1, 0), (2, 0)]

    def greeted(step):
        dx, dz = reach[step]
        for sign in (-1, 1):
            if dx:
                ok = gx + dx < N_GX if sign > 0 else gx >= dx
            else:
                ok = gz + dz < N_GZ if sign > 0 else gz >= dz
            yield ok, (gx + sign * dx, gz + sign * dz)

    def greet(step):
        for ok, peer in greeted(step):
            pl.when(ok)(
                lambda peer=peer: pl.semaphore_signal(
                    word_sem.at[step], inc=1, device_id=peer, device_id_type=MESH
                )
            )

    def heed(step):
        count = 0
        for ok, _ in greeted(step):
            count = count + ok.astype(jnp.int32)
        pl.semaphore_wait(word_sem.at[step], count)
        if step + 1 < len(reach):
            greet(step + 1)

    greet(0)

    def id_copy(sx, sz, peer=1):
        target = (1 - sx) * 3 + (1 - sz)
        return pltpu.make_async_remote_copy(
            ids.at[4], ids.at[target], id_send.at[target], id_recv.at[target],
            device_id=(gx + peer * sx, gz + peer * sz), device_id_type=MESH,
        )

    def layer_copy(number, peer=1):
        field, sx, sz, kx, kz, _ = MESSAGES[number]
        array = ls if field == "ls" else dv
        x_from, x_to, x_len = span(NX, X0, sx, *(kx or (0, 0)))
        z_from, z_to, z_len = span(NZ, Z0, sz, *(kz or (0, 0)))
        return pltpu.make_async_remote_copy(
            array.at[:, pl.ds(z_from, z_len), pl.ds(x_from, x_len)],
            array.at[:, pl.ds(z_to, z_len), pl.ds(x_to, x_len)],
            send_sem.at[number], recv_sem.at[number],
            device_id=(gx + peer * sx, gz + peer * sz), device_id_type=MESH,
        )

    def send(chosen):
        for number, message in enumerate(MESSAGES):
            if chosen(*message):
                _, sx, sz, _, _, _ = message
                pl.when(exists(sx, sz))(lambda number=number: layer_copy(number).start())

    def arrive(chosen):
        for number, message in enumerate(MESSAGES):
            if chosen(*message):
                _, sx, sz, _, _, _ = message
                pl.when(exists(-sx, -sz))(lambda number=number: layer_copy(number, -1).wait_recv())

    own_ids.wait()
    for sx, sz in around:
        pl.when(exists(sx, sz))(lambda sx=sx, sz=sz: id_copy(sx, sz).start())

    row = lax.broadcasted_iota(jnp.int32, (40, 1), 0)
    row_z = (row >= 10).astype(jnp.int32) + (row >= 20).astype(jnp.int32) + (row >= 30).astype(jnp.int32)
    row_x = row - 10 * row_z
    from_device = (
        jnp.where(row_x == 0, 0, jnp.where(row_x == 9, 2, 1)) * 3
        + jnp.where(row_z == 0, 0, jnp.where(row_z == 3, 2, 1))
    )
    tile_x = jnp.where(row_x == 0, 7, jnp.where(row_x == 9, 0, row_x - 1))
    tile_z = jnp.where(row_z == 0, 1, jnp.where(row_z == 3, 0, row_z - 1))
    code = tile_x * 2 + tile_z

    def listed(k, total):
        numbers = ids[k]
        wanted = jnp.where(from_device == k, code, -2)
        rows_hit = jnp.where((numbers >> 6) == wanted, 1.0, 0.0).astype(jnp.bfloat16)
        tile_y = lax.broadcasted_iota(jnp.int32, (64, 1), 0)
        y_hit = jnp.where((numbers & 63) == tile_y, 1.0, 0.0).astype(jnp.bfloat16)
        return total + lax.dot_general(
            rows_hit, y_hit, (((1,), (1,)), ((), ())), preferred_element_type=f32
        )

    widen = lax.broadcasted_iota(jnp.int32, (64, CH * LANES), 1) >> 3
    widen = jnp.where(widen == lax.broadcasted_iota(jnp.int32, (64, CH * LANES), 0), 1.0, 0.0)
    widen = widen.astype(jnp.bfloat16)

    def fill_table(first, last):
        tiles = lax.fori_loop(first, last, listed, jnp.zeros((40, 64), f32))
        cells = jnp.dot(tiles.astype(jnp.bfloat16), widen, preferred_element_type=f32)
        for c in range(CH):
            table[c] = cells[:, c * LANES : (c + 1) * LANES]

    def layer_of(p):
        return jnp.where(core == 1, p, PZ - 1 - p)

    def flat(ref):
        return ref.reshape(CH, PZ * PX, LANES)

    ls_f, dv_f, air_f, dist_f, gain_f, q1_f, q2_f, z0_f, y_f = map(
        flat, (ls, dv, air, dist, gain, q1, q2, z0_ref, y_ref)
    )
    lane = lax.broadcasted_iota(jnp.int32, (8, LANES), 1)

    def rows_at(ref, r):
        return [ref[c, pl.ds(r, 8), :] for c in range(CH)]

    def beside(ref, r, middle):
        up = [pltpu.roll(v, LANES - 1, 1) for v in middle]
        down = [pltpu.roll(v, 1, 1) for v in middle]
        pieces = []
        for c in range(CH):
            after = up[c + 1] if c + 1 < CH else 0.0
            before = down[c - 1] if c > 0 else 0.0
            pieces.append(
                [
                    ref[c, pl.ds(r + 1, 8), :],
                    ref[c, pl.ds(r - 1, 8), :],
                    ref[c, pl.ds(r + PX, 8), :],
                    ref[c, pl.ds(r - PX, 8), :],
                    jnp.where(lane == LANES - 1, after, up[c]),
                    jnp.where(lane == 0, before, down[c]),
                ]
            )
        return pieces

    def added(parts):
        a, b, c, d, e, f = parts
        return ((a + b) + (c + d)) + (e + f)

    def walk(first, last, layer, held=0, group=3):
        rounds = (last - first + 1) // group

        def some(q, held):
            for step in range(group):
                held = layer(layer_of(first + q * group + step), held)
            return held

        if rounds > 1:
            held = lax.fori_loop(0, rounds, some, held)
            first = first + rounds * group
        for p in range(first, last + 1):
            held = layer(layer_of(p), held)
        return held

    def find_air(columns):
        def layer(z, carry):
            base = z * PX
            row_of = 10 * (
                (z >= Z0).astype(jnp.int32)
                + (z >= Z0 + 8).astype(jnp.int32)
                + (z >= Z0 + 16).astype(jnp.int32)
            )
            for j in columns:
                for c in range(CH):
                    level = ls_f[c, pl.ds(base + 8 * j, 8), :]
                    on = table[c, pl.ds(row_of + j, 1), :] > 0.5
                    fluid = jnp.logical_and(level < 0, on)
                    air_f[c, pl.ds(base + 8 * j, 8), :] = jnp.where(fluid, 0.0, jnp.abs(level))
                    dist_f[c, pl.ds(base + 8 * j, 8), :] = jnp.where(fluid, -level, 0.0)
            return carry

        return layer

    def find_gain(columns, with_q1=True):
        def layer(z, carry):
            base = z * PX + 4
            for i in columns:
                r = base + 8 * i
                middle = rows_at(air_f, r)
                for c, parts in enumerate(beside(air_f, r, middle)):
                    distance = dist_f[c, pl.ds(r, 8), :]
                    most = 19.0 * distance
                    extra = added([jnp.minimum(part, most) for part in parts])
                    below = jnp.maximum(6.0 * distance + extra, 0.1)
                    here = (2.0 / 3.0) * distance / below
                    gain_f[c, pl.ds(r, 8), :] = here
                    if with_q1:
                        q1_f[c, pl.ds(r, 8), :] = here * dv_f[c, pl.ds(r, 8), :]
            return carry

        return layer

    def find_q1(z, carry):
        for i in (0, WALK - 1):
            r = z * PX + 4 + 8 * i
            for c in range(CH):
                q1_f[c, pl.ds(r, 8), :] = gain_f[c, pl.ds(r, 8), :] * dv_f[c, pl.ds(r, 8), :]
        return carry

    def stage(source, target, own_part, sign, columns=range(WALK)):
        def layer(z, carry):
            base = z * PX + 4
            for i in columns:
                r = base + 8 * i
                middle = rows_at(source, r)
                for c, parts in enumerate(beside(source, r, middle)):
                    here = gain_f[c, pl.ds(r, 8), :] * added(parts)
                    target[c, pl.ds(r, 8), :] = own_part * middle[c] + sign * here
            return carry

        return layer

    def find_z0(columns=range(WALK)):
        return stage(q1_f, z0_f, 4.0 / 3.0, 1.0, columns)

    def find_q2(columns=range(WALK)):
        return stage(z0_f, q2_f, 2.0 / 3.0, -1.0, columns)

    find_y = stage(q2_f, y_f, 4.0 / 3.0, 1.0)

    def finish(z, held):
        base = z * PX + X0
        out = (z - Z0) * NX
        held = list(held)
        for i in range(NX // 8):
            r = base + 8 * i
            middle = rows_at(y_f, r)
            for c, parts in enumerate(beside(y_f, r, middle)):
                here = gain_f[c, pl.ds(r, 8), :]
                inverse = 1.0 / jnp.maximum(here, 1e-3)
                r0 = jnp.where(here > 0.0, dv_f[c, pl.ds(r, 8), :], 0.0)
                w0 = inverse * q2_f[c, pl.ds(r, 8), :]
                u = inverse * ((2.0 / 3.0) * middle[c] - here * added(parts))
                z0 = z0_f[c, pl.ds(r, 8), :]
                y = middle[c]
                r0_ref[c, pl.ds(out + 8 * i, 8), :] = r0
                w0_ref[c, pl.ds(out + 8 * i, 8), :] = w0
                u_ref[c, pl.ds(out + 8 * i, 8), :] = u
                z_s = z0 - SHIFT * y
                products = (r0 * z0, w0 * z0, r0 * z_s, w0 * z_s, u * z_s)
                held = [total + term for total, term in zip(held, products)]
        return tuple(held)

    from_above = lambda sz: sz == -1
    from_below = lambda sz: sz == 1

    def arrive_at(side_of_even, side_of_odd, chosen):
        for parity, side in ((0, side_of_even), (1, side_of_odd)):

            @pl.when(core == parity)
            def _(side=side):
                arrive(lambda field, sx, sz, kx, kz, wave: side(sz) and chosen(field, sx, wave))

    def arrive_early(chosen):
        arrive_at(from_above, from_below, chosen)

    def arrive_late(chosen):
        arrive_at(from_below, from_above, chosen)

    every_column, inner = range(10), range(1, 9)
    edges, between = (0, WALK - 1), range(1, WALK - 1)
    fill_table(4, 5)
    loaded(ls, 0, (0, 1))
    send(lambda field, sx, sz, kx, kz, wave: field == "ls" and sx == 0 and wave == 1)
    loaded(ls, 0, (2,))
    send(lambda field, sx, sz, kx, kz, wave: field == "ls" and sx != 0 and sz == 0)
    send(lambda field, sx, sz, kx, kz, wave: field == "ls" and sx != 0 and sz != 0)
    walk(5, 20, find_air(inner))
    loaded(dv, 1, (0, 1))
    send(lambda field, sx, sz, kx, kz, wave: field == "dv" and sx == 0 and wave == 1)
    loaded(dv, 1, (2,))
    send(lambda field, sx, sz, kx, kz, wave: field == "dv" and sx != 0 and sz == 0)
    send(lambda field, sx, sz, kx, kz, wave: field == "dv" and sx != 0 and sz != 0)
    send(lambda field, sx, sz, kx, kz, wave: wave == 2)
    heed(0)
    walk(6, 19, find_gain(between))
    heed(1)
    for sx, sz in around:
        pl.when(exists(-sx, -sz))(lambda sx=sx, sz=sz: id_copy(sx, sz, -1).wait_recv())
    fill_table(0, 9)
    arrive_early(lambda field, sx, wave: sx == 0)
    walk(0, 4, find_air(inner))
    walk(1, 5, find_gain(between))
    heed(2)
    arrive(lambda field, sx, sz, kx, kz, wave: sz == 0 and field == "ls")
    arrive_early(lambda field, sx, wave: sx != 0 and field == "ls")
    walk(0, 20, find_air((0, 9)))
    walk(1, 19, find_gain(edges, False))
    heed(3)
    walk(2, 18, find_z0(range(2, 7)), group=6)
    walk(3, 17, find_q2(range(3, 6)), group=5)
    arrive(lambda field, sx, sz, kx, kz, wave: sz == 0 and field == "dv")
    arrive_early(lambda field, sx, wave: sx != 0 and field == "dv")
    heed(4)
    walk(1, 19, find_q1)
    walk(2, 18, find_z0((0, 1, 7, 8)), group=6)
    walk(3, 17, find_q2((0, 1, 2, 6, 7, 8)), group=5)
    heed(5)
    walk(4, 16, find_y, group=5)
    held = walk(5, 15, finish, tuple(jnp.zeros((8, LANES), f32) for _ in range(5)), group=3)

    heed(6)
    arrive_late(lambda field, sx, wave: wave == 1)
    walk(21, 24, find_air(every_column), group=2)
    walk(20, 23, find_gain(range(WALK)), group=2)
    walk(19, 22, find_z0(), group=4)
    walk(18, 21, find_q2(), group=4)
    walk(17, 20, find_y, group=4)
    held = walk(16, 19, finish, held, group=2)

    arrive_late(lambda field, sx, wave: wave == 2)
    walk(25, 25, find_air(every_column))
    walk(24, 24, find_gain(range(WALK)))
    walk(23, 23, find_z0())
    walk(22, 22, find_q2())
    walk(21, 21, find_y)
    held = walk(20, 20, finish, held)

    lane_row = lax.broadcasted_iota(jnp.int32, (1, LANES), 1)
    packed = jnp.zeros((1, LANES), f32)
    for k, total in enumerate(held):
        whole = jnp.sum(jnp.sum(total, axis=0, keepdims=True), axis=1, keepdims=True)
        packed = jnp.where(lane_row == k, whole, packed)

    def ring_distance(i):
        return sum((0, 1, 2, 1)[(i >> shift) & 3] for shift in (1, 3, 5))

    every_sum[pl.ds(0, 1), :] = packed
    for i in sorted(range(1, DEVICES), key=lambda i: -ring_distance(i)):
        pltpu.make_async_remote_copy(
            every_sum.at[pl.ds(0, 1)], every_sum.at[pl.ds(i, 1)], ar_send.at[0], ar_recv.at[0],
            device_id=sum_peer(i), device_id_type=MESH,
        ).start()
    sent = pltpu.make_async_remote_copy(
        every_sum.at[pl.ds(0, DEVICES - 1)], every_sum.at[pl.ds(1, DEVICES - 1)], ar_send.at[0], ar_recv.at[0],
        device_id=sum_peer(1), device_id_type=MESH,
    )
    sent.wait_recv()
    sums[pl.ds(0, 1), :] = jnp.sum(every_sum[...], axis=0, keepdims=True)
    gamma0, delta0, first, kappa, lam = (sums[pl.ds(0, 1), pl.ds(k, 1)] for k in range(5))
    eta = (delta0 - kappa) / SHIFT
    theta = (eta - lam) / SHIFT
    gamma_s, delta_s = first - SHIFT * kappa, kappa - SHIFT * lam
    alpha0 = gamma0 / delta0
    off = alpha0 - SHIFT
    gamma1 = gamma_s - 2.0 * off * kappa + off * off * eta
    delta1 = delta_s - 2.0 * off * lam + off * off * theta
    beta = gamma1 / gamma0
    below = delta1 - beta * gamma1 / alpha0
    alpha1 = jnp.where(below > 0, gamma1 / jnp.where(below > 0, below, 1.0), 0.0)
    for k, value in enumerate((alpha0, alpha1, beta)):
        step_ref[k] = jnp.broadcast_to(value, (8, LANES))

    for number, message in enumerate(MESSAGES):
        _, sx, sz, _, _, _ = message
        pl.when(exists(sx, sz))(lambda number=number: layer_copy(number).wait_send())
    for sx, sz in around:
        pl.when(exists(sx, sz))(lambda sx=sx, sz=sz: id_copy(sx, sz).wait_send())
    sent.wait_send()


def last_kernel(z0_ref, y_ref, r0_ref, w0_ref, u_ref, step_ref, p_out, r_out, p_buf, r_buf, sem):
    alpha0, alpha1, beta = step_ref[0], step_ref[1], step_ref[2]
    z0_f = z0_ref.reshape(CH, PZ * PX, LANES)
    y_f = y_ref.reshape(CH, PZ * PX, LANES)
    p_f = p_buf.reshape(CH, NZ * NX, LANES)
    r_f = r_buf.reshape(CH, NZ * NX, LANES)

    for z in range(NZ):
        def rows(i, carry, z=z):
            wide = (Z0 + z) * PX + X0 + 8 * i
            r = z * NX + 8 * i
            for c in range(CH):
                z0 = z0_f[c, pl.ds(wide, 8), :]
                z1 = z0 - alpha0 * y_f[c, pl.ds(wide, 8), :]
                p_f[c, pl.ds(r, 8), :] = alpha0 * z0 + alpha1 * (z1 + beta * z0)
                w0 = w0_ref[c, pl.ds(r, 8), :]
                w1 = w0 - alpha0 * u_ref[c, pl.ds(r, 8), :]
                r1 = r0_ref[c, pl.ds(r, 8), :] - alpha0 * w0
                r_f[c, pl.ds(r, 8), :] = r1 - alpha1 * (w1 + beta * w0)
            return carry

        lax.fori_loop(0, NX // 8, rows, 0, unroll=True)
        for number, (buffer, target) in enumerate(((p_buf, p_out), (r_buf, r_out))):
            for c in range(CH):
                pltpu.make_async_copy(
                    buffer.at[c, z], target.at[:, z, pl.ds(c * LANES, LANES)], sem.at[number]
                ).start()
    for number, buffer in enumerate((p_buf, r_buf)):
        pltpu.make_async_copy(buffer, buffer, sem.at[number]).wait()


def on_device(divergence, level_set, tile_ids):
    extended = (CH, PZ, PX, LANES)
    block = (CH, NZ * NX, LANES)
    held = pl.pallas_call(
        main_kernel,
        out_shape=[pltpu.VMEM(extended, f32)] * 2 + [pltpu.VMEM(block, f32)] * 3 + [pltpu.VMEM((3, 8, LANES), f32)],
        in_specs=[pl.BlockSpec(memory_space=pltpu.HBM)] * 3,
        out_specs=[pl.BlockSpec(memory_space=pltpu.VMEM)] * 6,
        scratch_shapes=[
            *[pltpu.VMEM(extended, f32)] * 7,
            pltpu.VMEM((9, 1, SLOTS), jnp.int32),
            pltpu.VMEM((CH, 40, LANES), f32),
            pltpu.VMEM((8, LANES), f32),
            pltpu.VMEM((DEVICES, LANES), f32),
            pltpu.SemaphoreType.DMA((7,)),
            pltpu.SemaphoreType.DMA((len(MESSAGES),)),
            pltpu.SemaphoreType.DMA((len(MESSAGES),)),
            pltpu.SemaphoreType.DMA((9,)),
            pltpu.SemaphoreType.DMA((9,)),
            pltpu.SemaphoreType.DMA((1,)),
            pltpu.SemaphoreType.DMA((1,)),
            pltpu.SemaphoreType.REGULAR((7,)),
        ],
        compiler_params=pltpu.CompilerParams(
            collective_id=0, has_side_effects=True, vmem_limit_bytes=40 * 2**20
        ),
        name="solve",
    )(*(pltpu.with_memory_space_constraint(array, pltpu.HBM) for array in (divergence, level_set, tile_ids)))
    return pl.pallas_call(
        last_kernel,
        out_shape=[jax.ShapeDtypeStruct(divergence.shape, f32)] * 2,
        in_specs=[pl.BlockSpec(memory_space=pltpu.VMEM)] * 6,
        out_specs=[pl.BlockSpec(memory_space=pl.ANY)] * 2,
        scratch_shapes=[
            pltpu.VMEM((CH, NZ, NX, LANES), f32),
            pltpu.VMEM((CH, NZ, NX, LANES), f32),
            pltpu.SemaphoreType.DMA((2,)),
        ],
        compiler_params=pltpu.CompilerParams(vmem_limit_bytes=12 * 2**20),
        name="update",
    )(*held)


def solution(mesh):
    return jax.shard_map(
        on_device,
        mesh=mesh,
        in_specs=(P("gx", "gz", None), P("gx", "gz", None), P("gx", "gz")),
        out_specs=(P("gx", "gz", None), P("gx", "gz", None)),
        check_vma=False,
    )
```
